128 devices in a mesh: section: 8 (over y_hi, z), dp: 16 (over x, y_lo, core).
Axes of the slice: x: 4, y: 4 (y_hi: 2, y_lo: 2; y = y_hi * 2 + y_lo), z: 4, core: 2. Of those that a mesh axis runs over, the one named last changes fastest.
Arguments:
- activations: bfloat16 [8, 4, 4096, 1280], P('section', None, 'dp'), may hold values from -6 to 6
- cotangent: bfloat16 [4, 4096, 1280], P(None, 'dp'), may hold values from -1.5 to 1.5
- counts: int32 [4, 16], P(None, 'dp'), may hold values from 64 to 256
- arrival: int32 [4], replicated, may hold values from 0 to 3, each once
- norm_gain: float32 [8, 1280], P('section'), may hold values from 0.1 to 1.9
- qkv_weight: bfloat16 [8, 1280, 1920], P('section'), may hold values from -8 to 8
- out_weight: bfloat16 [8, 1280, 640], P('section'), may hold values from -0.25 to 0.25
Outputs:
- qkv_grad: float32 [8, 1280, 1920], P('section', 'dp')
- out_grad: float32 [8, 1280, 640], P('section', 'dp')
The draws below stay inside these ranges and needn't reach their ends.
Inputs may be any that keep to these rules, and one draw needn't show every extreme that they name: `arrival`: each microbatch once.
All inputs are finite; a program needn't handle non-finite values.
Results may differ from the reference program's by a relative error of at most 0.025.
Values may be sent and summed in bfloat16 or wider, within the bound.
A program may use at most 128 MiB of HBM per device.

```python
import math
import jax
import jax.numpy as jnp
from jax import lax

D = 1280
HDIM = 80
HEADS = 8
SLOTS = 256
MICRO = 4
LAYERS = 8
HD = 640
QKV = 1920
ROWS = 4096
N_DP = 16


def draw_qkv_weight(key, part):
    base_key = jax.random.fold_in(jax.random.fold_in(key, 11), 0)
    head_span = HEADS * HDIM
    drawn = jax.random.normal(base_key, (LAYERS, D, 3 * head_span), jnp.float32) / math.sqrt(D)
    return jnp.clip(drawn, -8.0, 8.0).astype(jnp.bfloat16)


def touch_ends(entries, stream_key, smallest, largest):
    extent = entries.shape
    spot = [jax.random.randint(jax.random.fold_in(stream_key, axis), (), 0, extent[axis]) for axis in range(len(extent))]
    entries = entries.at[tuple(spot)].set(smallest)
    longest = extent.index(max(extent))
    spot[longest] = (spot[longest] + 1) % extent[longest]
    return entries.at[tuple(spot)].set(largest)


def levels(rng, shape, cuts, least, high):
    gain = 1.0
    for axis_at, blocks in cuts:
        steps = jax.random.uniform(jax.random.fold_in(jax.random.fold_in(rng, 6), axis_at), (blocks,), jnp.float32, least / len(cuts), high / len(cuts))
        gain = gain * jnp.repeat(jnp.exp(steps), shape[axis_at] // blocks).reshape((-1,) + (1,) * (len(shape) - 1 - axis_at))
    return gain


def scatter_about(rng, extent, deviation, most, cuts=(), held_as=jnp.bfloat16):
    factor_of = levels(rng, extent, cuts, -0.22, 0.18) if cuts else 1.0
    values = jax.random.normal(rng, extent, jnp.float32) * deviation * factor_of
    return jnp.minimum(jnp.maximum(values, -most), most).astype(held_as)


def setup_inputs(seed: int = 0) -> dict:
    seeds = jax.random.split(jax.random.key(seed), 8)
    return {
        "activations": scatter_about(seeds[0], (LAYERS, MICRO, ROWS, D), 1.0, 6.0, ((0, 8), (2, 16))),
        "cotangent": scatter_about(seeds[1], (MICRO, ROWS, D), 0.25, 1.5, ((1, 16),)),
        "counts": touch_ends(jax.random.randint(seeds[2], (MICRO, N_DP), SLOTS // 4, SLOTS + 1), jax.random.fold_in(seeds[2], 1), SLOTS // 4, SLOTS).astype(jnp.int32),
        "arrival": jax.random.permutation(seeds[3], MICRO).astype(jnp.int32),
        "norm_gain": jnp.clip(1.0 + 0.18 * jax.random.normal(seeds[4], (LAYERS, D), jnp.float32), 0.1, 1.9),
        "qkv_weight": draw_qkv_weight(jax.random.fold_in(seeds[7], 71), 0),
        "out_weight": scatter_about(seeds[6], (LAYERS, D, HD), HD ** -0.5, 0.25, ((0, 8),)),
    }


EPSILON = 1e-06

def recompute(inputs, visible, gain_row, w_qkv):
    slot_count = inputs.shape[0]
    floats = inputs.astype(jnp.float32)
    centered = floats - lax.optimization_barrier(jnp.mean(floats, axis=-1, keepdims=True))
    inv_std = lax.rsqrt(lax.optimization_barrier(jnp.mean(centered * centered, axis=-1, keepdims=True)) + EPSILON)
    normed = centered * inv_std
    hidden = (normed * gain_row).astype(jnp.bfloat16)
    packed = jnp.dot(hidden, w_qkv, preferred_element_type=jnp.float32).astype(jnp.bfloat16)
    head_span = packed.shape[1] // 3
    queries = packed[:, :head_span].reshape(slot_count, HEADS, HDIM)
    keys_all = packed[:, head_span:2 * head_span].reshape(slot_count, HEADS, HDIM)
    values_all = packed[:, 2 * head_span:].reshape(slot_count, HEADS, HDIM)
    scores = jnp.einsum('ihd,jhd->hij', queries.astype(jnp.float32), keys_all.astype(jnp.float32)) * HDIM ** (-0.5)
    keep = jnp.arange(slot_count) < visible
    scores = jnp.where(keep[None, None, :], scores, -1e+30)
    row_max = lax.optimization_barrier(jnp.max(scores, axis=-1, keepdims=True))
    exp_scores = jnp.exp(scores - row_max)
    prob_full = exp_scores / lax.optimization_barrier(jnp.sum(exp_scores, axis=-1, keepdims=True))
    prob_half = prob_full.astype(jnp.bfloat16)
    attn_out = jnp.einsum('hij,jhd->ihd', prob_half.astype(jnp.float32), values_all.astype(jnp.float32))
    attn_out = attn_out.reshape(slot_count, head_span).astype(jnp.bfloat16)
    return (normed, inv_std, hidden, queries, keys_all, values_all, prob_full, prob_half, attn_out, keep)

def backward_layer(inputs, grad_out, visible, gain_row, w_qkv, w_out):
    slot_count = inputs.shape[0]
    normed, inv_std, hidden, queries, keys_all, values_all, prob_full, prob_half, attn_out, keep = recompute(inputs, visible, gain_row, w_qkv)
    head_span = attn_out.shape[1]
    masked = jnp.where(keep[:, None], grad_out, jnp.zeros_like(grad_out))
    out_part = jnp.dot(masked.T, attn_out, preferred_element_type=jnp.float32)
    grad_attn = jnp.dot(masked, w_out, preferred_element_type=jnp.float32).astype(jnp.bfloat16)
    grad_attn = grad_attn.reshape(slot_count, HEADS, HDIM).astype(jnp.float32)
    grad_prob = jnp.einsum('ihd,jhd->hij', grad_attn, values_all.astype(jnp.float32))
    grad_values = jnp.einsum('hij,ihd->jhd', prob_half.astype(jnp.float32), grad_attn)
    inner = lax.optimization_barrier(jnp.sum(prob_full * grad_prob, axis=-1, keepdims=True))
    grad_scores = (prob_full * (grad_prob - inner) * HDIM ** (-0.5)).astype(jnp.bfloat16).astype(jnp.float32)
    grad_queries = jnp.einsum('hij,jhd->ihd', grad_scores, keys_all.astype(jnp.float32))
    grad_keys = jnp.einsum('hij,ihd->jhd', grad_scores, queries.astype(jnp.float32))
    grad_packed = jnp.concatenate([grad_queries.reshape(slot_count, head_span), grad_keys.reshape(slot_count, head_span), grad_values.reshape(slot_count, head_span)], axis=1).astype(jnp.bfloat16)
    qkv_part = jnp.dot(hidden.T, grad_packed, preferred_element_type=jnp.float32)
    grad_hidden = jnp.dot(grad_packed, w_qkv.T, preferred_element_type=jnp.float32)
    grad_normed = grad_hidden * gain_row
    grad_ln = inv_std * (grad_normed - lax.optimization_barrier(jnp.mean(grad_normed, axis=-1, keepdims=True)) - normed * lax.optimization_barrier(jnp.mean(grad_normed * normed, axis=-1, keepdims=True)))
    grad_in = (masked.astype(jnp.float32) + grad_ln).astype(jnp.bfloat16)
    return (grad_in, qkv_part, out_part)

def reference(activations, cotangent, counts, arrival, norm_gain, qkv_weight, out_weight):
    layer_total = activations.shape[0]
    micro_count = cotangent.shape[0]
    batched = jax.vmap(backward_layer, in_axes=(0, 0, 0, None, None, None))
    flowing = [cotangent[position].reshape(N_DP, SLOTS, D) for position in range(micro_count)]
    qkv_list = []
    out_list = []
    for layer_idx in reversed(range(layer_total)):
        qkv_total = jnp.zeros((D, QKV), jnp.float32)
        out_total = jnp.zeros((D, HD), jnp.float32)
        for position in range(micro_count):
            chosen = arrival[position]
            inputs = activations[layer_idx, chosen].reshape(N_DP, SLOTS, D)
            grad_in, qkv_part, out_part = batched(inputs, flowing[position], counts[chosen], norm_gain[layer_idx], qkv_weight[layer_idx], out_weight[layer_idx])
            qkv_total = qkv_total + lax.optimization_barrier(jnp.sum(qkv_part, axis=0))
            out_total = out_total + lax.optimization_barrier(jnp.sum(out_part, axis=0))
            flowing[position] = grad_in
        qkv_list.insert(0, qkv_total)
        out_list.insert(0, out_total)
    return (jnp.stack(qkv_list), jnp.stack(out_list))
```

```python
import functools

import jax
import jax.numpy as jnp
from jax import lax
from jax.experimental import pallas as pl
from jax.experimental.pallas import tpu as pltpu
from jax.sharding import PartitionSpec as P

HDIM = 80
HEADS = 8
EPSILON = 1e-06
MESH = pl.DeviceIdType.MESH
F32 = jnp.float32
BF16 = jnp.bfloat16


def dot_nn(a, b):
    return lax.dot_general(a, b, (((1,), (0,)), ((), ())), preferred_element_type=F32)


def dot_nt(a, b):
    return lax.dot_general(a, b, (((1,), (1,)), ((), ())), preferred_element_type=F32)


def loop(count, body):
    def step(i, carry):
        body(i)
        return carry

    lax.fori_loop(0, count, step, 0)


def rows_at(i, size):
    return pl.ds(pl.multiple_of(i * size, size), size)


def pipeline_kernel(
    sections,
    counts_ref,
    arrival_ref,
    x_ref,
    cot_ref,
    gain_ref,
    wqkv_ref,
    wo_ref,
    out_ref,
    wqkv_t,
    wo_t,
    gain_b,
    x_t,
    norm_t,
    hid_t,
    stats,
    pk_t,
    v_n,
    prob_f,
    prob_h,
    attn_t,
    ga_t,
    gpk_t,
    gn_t,
    acc_q,
    acc_o,
    g_recv,
    g_send,
    send_sem,
    recv_sem,
):
    micro, slots, width = x_ref.shape
    head_span = wo_ref.shape[1]
    packed = wqkv_ref.shape[1]
    scale = HDIM**-0.5
    sec = lax.axis_index("section")
    below = lax.rem(sec + sections - 1, sections)
    above = lax.rem(sec + 1, sections)
    barrier = pltpu.get_barrier_semaphore()
    for other in (below, above):
        pl.semaphore_signal(barrier, inc=1, device_id={"section": other}, device_id_type=MESH)
    pl.semaphore_wait(barrier, 2)

    def turn_wo(c):
        wo_t[:, rows_at(c, 256)] = wo_ref[rows_at(c, 256), :].T

    def turn_wqkv(c):
        wqkv_t[:, rows_at(c, 256)] = wqkv_ref[rows_at(c, 256), :].T

    loop(width // 256, turn_wqkv)
    loop(width // 256, turn_wo)
    gain_b[...] = jnp.broadcast_to(gain_ref[...], (128, width)).T

    CH = 160
    chunks = width // CH

    def gain_rows(c, size):
        part = gain_b[rows_at(c, size), :]
        return jnp.concatenate([part] * (slots // 128), axis=1)

    def forward(p):
        chosen = arrival_ref[p]
        count = counts_ref[chosen]

        def turn(c):
            x_t[rows_at(c, 256), :] = x_ref[chosen, :, rows_at(c, 256)].T

        loop(width // 256, turn)

        def add(c, total):
            return total + jnp.sum(x_t[rows_at(c, CH), :].astype(F32), axis=0, keepdims=True)

        zero = jnp.zeros((1, slots), F32)
        mean = lax.fori_loop(0, chunks, add, zero) * (1.0 / width)

        def add_sq(c, total):
            centered = x_t[rows_at(c, CH), :].astype(F32) - mean
            return total + jnp.sum(centered * centered, axis=0, keepdims=True)

        var = lax.fori_loop(0, chunks, add_sq, zero) * (1.0 / width)
        inv = lax.rsqrt(var + EPSILON)
        stats[0:1, :] = inv

        def norm(c):
            normed = (x_t[rows_at(c, CH), :].astype(F32) - mean) * inv
            norm_t[rows_at(c, CH), :] = normed
            hid_t[rows_at(c, CH), :] = (normed * gain_rows(c, CH)).astype(BF16)

        loop(chunks, norm)

        def pack(m):
            pk_t[rows_at(m, 480), :] = dot_nn(wqkv_t[rows_at(m, 480), :], hid_t[...]).astype(BF16)

        loop(packed // 480, pack)
        keep = lax.broadcasted_iota(jnp.int32, (slots, slots), 0) < count

        def head(h):
            q = pk_t[rows_at(h, HDIM), :]
            k = pk_t[rows_at(h + HEADS, HDIM), :]
            v = pk_t[rows_at(h + 2 * HEADS, HDIM), :]
            s = dot_nn(k.T, q) * scale
            s = jnp.where(keep, s, -1e30)
            e = jnp.exp(s - jnp.max(s, axis=0, keepdims=True))
            prob = e * (1.0 / jnp.sum(e, axis=0, keepdims=True))
            prob_f[h] = prob
            half = prob.astype(BF16)
            prob_h[h] = half
            v_n[h] = v.T
            attn_t[rows_at(h, HDIM), :] = dot_nn(v, half).astype(BF16)

        loop(HEADS, head)

    def take_cotangent(p):
        count = counts_ref[arrival_ref[p]]
        keep = (lax.broadcasted_iota(jnp.int32, (1, slots), 1) < count).astype(F32)

        def turn(c):
            piece = cot_ref[p, :, rows_at(c, 256)].T.astype(F32) * keep
            g_recv[p, rows_at(c, 256), :] = piece.astype(BF16)

        loop(width // 256, turn)

    def hop(p):
        return pltpu.make_async_remote_copy(
            src_ref=g_send.at[p],
            dst_ref=g_recv.at[p],
            send_sem=send_sem.at[p],
            recv_sem=recv_sem.at[p],
            device_id={"section": below},
            device_id_type=MESH,
        )

    def backward(p):
        def grad_attn(m):
            ga_t[rows_at(m, 320), :] = dot_nn(wo_t[rows_at(m, 320), :], g_recv[p]).astype(BF16)

        loop(head_span // 320, grad_attn)

        def head(h):
            q = pk_t[rows_at(h, HDIM), :]
            k = pk_t[rows_at(h + HEADS, HDIM), :]
            ga = ga_t[rows_at(h, HDIM), :]
            prob = prob_f[h]
            grad_prob = dot_nn(v_n[h], ga)
            inner = jnp.sum(prob * grad_prob, axis=0, keepdims=True)
            gs = (prob * (grad_prob - inner) * scale).astype(BF16)
            gpk_t[rows_at(h, HDIM), :] = dot_nn(k, gs).astype(BF16)
            gpk_t[rows_at(h + HEADS, HDIM), :] = dot_nt(q, gs).astype(BF16)
            gpk_t[rows_at(h + 2 * HEADS, HDIM), :] = dot_nt(ga, prob_h[h]).astype(BF16)

        loop(HEADS, head)

    def pass_down(p):
        def grad_hidden(m, sums):
            gn = dot_nn(wqkv_ref[rows_at(m, 320), :], gpk_t[...]) * gain_rows(m, 320)
            gn_t[rows_at(m, 320), :] = gn
            return (
                sums[0] + jnp.sum(gn, axis=0, keepdims=True),
                sums[1] + jnp.sum(gn * norm_t[rows_at(m, 320), :], axis=0, keepdims=True),
            )

        zero = jnp.zeros((1, slots), F32)
        first, second = lax.fori_loop(0, width // 320, grad_hidden, (zero, zero))
        first = first * (1.0 / width)
        second = second * (1.0 / width)
        inv = stats[0:1, :]

        def finish(c):
            at = rows_at(c, CH)
            grad_ln = inv * (gn_t[at, :] - first - norm_t[at, :] * second)
            g_send[p, at, :] = (g_recv[p, at, :].astype(F32) + grad_ln).astype(BF16)

        loop(chunks, finish)
        hop(p).start()

    def weights(p):
        def qkv(n):
            acc_q[:, rows_at(n, 256)] += dot_nt(hid_t[...], gpk_t[rows_at(n, 256), :])

        loop(packed // 256, qkv)
        tail = packed // 256 * 256
        acc_q[:, tail:packed] += dot_nt(hid_t[...], gpk_t[tail:packed, :])

        def out(n):
            acc_o[:, rows_at(n, 256)] += dot_nt(g_recv[p], attn_t[rows_at(n, 256), :])

        loop(head_span // 256, out)
        tail = head_span // 256 * 256
        acc_o[:, tail:head_span] += dot_nt(g_recv[p], attn_t[tail:head_span, :])

    def clear(c):
        acc_q[rows_at(c, 64), :] = jnp.zeros((64, packed), F32)
        acc_o[rows_at(c, 64), :] = jnp.zeros((64, head_span), F32)

    forward(0)

    def moment(p):
        @pl.when(sec == sections - 1)
        def _():
            take_cotangent(p)

        @pl.when(sec < sections - 1)
        def _():
            hop(p).wait_recv()

        backward(p)

        @pl.when(sec > 0)
        def _():
            pass_down(p)

        @pl.when(p == 0)
        def _():
            loop(width // 64, clear)

        weights(p)

        @pl.when(p < micro - 1)
        def _():
            forward(p + 1)

    loop(micro, moment)

    @pl.when(sec > 0)
    def _():
        def drain(p):
            hop(p).wait_send()

        loop(micro, drain)

    def finish(c):
        out_ref[rows_at(c, 64), 0:packed] = acc_q[rows_at(c, 64), :].astype(BF16)
        out_ref[rows_at(c, 64), packed:] = acc_o[rows_at(c, 64), :].astype(BF16)

    loop(width // 64, finish)


def run_pipeline(sections, counts, arrival, x, cotangent, gain, wqkv, wo):
    micro, slots, width = x.shape
    packed, head_span = wqkv.shape[1], wo.shape[1]
    vmem = pl.BlockSpec(memory_space=pltpu.VMEM)
    smem = pl.BlockSpec(memory_space=pltpu.SMEM)
    scratch = [
        pltpu.VMEM((packed, width), BF16),
        pltpu.VMEM((head_span, width), BF16),
        pltpu.VMEM((width, 128), F32),
        pltpu.VMEM((width, slots), BF16),
        pltpu.VMEM((width, slots), F32),
        pltpu.VMEM((width, slots), BF16),
        pltpu.VMEM((8, slots), F32),
        pltpu.VMEM((packed, slots), BF16),
        pltpu.VMEM((HEADS, slots, HDIM), BF16),
        pltpu.VMEM((HEADS, slots, slots), F32),
        pltpu.VMEM((HEADS, slots, slots), BF16),
        pltpu.VMEM((head_span, slots), BF16),
        pltpu.VMEM((head_span, slots), BF16),
        pltpu.VMEM((packed, slots), BF16),
        pltpu.VMEM((width, slots), F32),
        pltpu.VMEM((width, packed), F32),
        pltpu.VMEM((width, head_span), F32),
        pltpu.VMEM((micro, width, slots), BF16),
        pltpu.VMEM((micro, width, slots), BF16),
        pltpu.SemaphoreType.DMA((micro,)),
        pltpu.SemaphoreType.DMA((micro,)),
    ]
    return pl.pallas_call(
        functools.partial(pipeline_kernel, sections),
        out_shape=jax.ShapeDtypeStruct((width, packed + head_span), BF16),
        in_specs=[smem, smem, vmem, vmem, vmem, vmem, vmem],
        out_specs=vmem,
        scratch_shapes=scratch,
        compiler_params=pltpu.CompilerParams(
            collective_id=0, has_side_effects=True, vmem_limit_bytes=64 * 1024 * 1024 - 65536
        ),
        name="pipeline",
    )(counts, arrival, x, cotangent, gain, wqkv, wo)


def per_device(activations, cotangent, counts, arrival, norm_gain, qkv_weight, out_weight):
    sections = lax.axis_size("section")
    packed = qkv_weight.shape[2]
    both = run_pipeline(
        sections,
        counts[:, 0],
        arrival,
        activations[0],
        cotangent,
        norm_gain,
        qkv_weight[0],
        out_weight[0],
    )
    share = lax.psum_scatter(both, "dp", scatter_dimension=0, tiled=True).astype(F32)
    return (share[None, :, :packed], share[None, :, packed:])


def solution(mesh):
    placed = (
        P("section", None, "dp", None),
        P(None, "dp", None),
        P(None, "dp"),
        P(),
        P("section", None),
        P("section", None, None),
        P("section", None, None),
    )
    return jax.shard_map(
        per_device,
        mesh=mesh,
        in_specs=placed,
        out_specs=(P("section", "dp", None), P("section", "dp", None)),
        check_vma=False,
    )
```

```python
import functools

import jax
import jax.numpy as jnp
from jax import lax
from jax.experimental import pallas as pl
from jax.experimental.pallas import tpu as pltpu
from jax.sharding import PartitionSpec as P

HDIM = 80
HEADS = 8
EPSILON = 1e-06
MESH = pl.DeviceIdType.MESH
F32 = jnp.float32
BF16 = jnp.bfloat16


def dot_nn(a, b):
    return lax.dot_general(a, b, (((1,), (0,)), ((), ())), preferred_element_type=F32)


def dot_nt(a, b):
    return lax.dot_general(a, b, (((1,), (1,)), ((), ())), preferred_element_type=F32)


def fold(a):
    return jnp.sum(a.reshape(a.shape[0] // 8, 8, a.shape[1]), axis=0)


def loop(count, body):
    def step(i, carry):
        body(i)
        return carry

    lax.fori_loop(0, count, step, 0)


def rows_at(i, size):
    if isinstance(i, int):
        return pl.ds(i * size, size)
    return pl.ds(pl.multiple_of(i * size, size), size)


def pipeline_kernel(
    sections,
    counts_ref,
    arrival_ref,
    x_ref,
    cot_ref,
    gain_ref,
    wqkv_ref,
    wo_ref,
    out_ref,
    wqkv_t,
    wo_t,
    gain_b,
    x_t,
    norm_t,
    hid_t,
    stats,
    pk_t,
    v_n,
    prob_f,
    prob_h,
    attn_t,
    ga_t,
    ga_acc,
    gpk_t,
    gain_w,
    acc_q,
    acc_o,
    g_recv,
    g_send,
    send_sem,
    recv_sem,
    go_sem,
):
    micro, slots, width = x_ref.shape
    head_span = wo_ref.shape[1]
    packed = wqkv_ref.shape[1]
    scale = HDIM**-0.5
    sec = lax.axis_index("section")
    below = lax.rem(sec + sections - 1, sections)
    above = lax.rem(sec + 1, sections)
    lane = lax.axis_index("dp")
    core = lax.rem(lane, 2)
    twin = lane + 1 - 2 * core
    barrier = pltpu.get_barrier_semaphore()
    for other in (below, above):
        pl.semaphore_signal(barrier, inc=1, device_id={"section": other}, device_id_type=MESH)
    pl.semaphore_signal(barrier, inc=1, device_id={"dp": twin}, device_id_type=MESH)
    pl.semaphore_wait(barrier, 3)

    def turn_wo(c):
        wo_t[:, rows_at(c, 256)] = wo_ref[rows_at(c, 256), :].T

    def turn_wqkv(c):
        wqkv_t[:, rows_at(c, 256)] = wqkv_ref[rows_at(c, 256), :].T

    loop(width // 256, turn_wqkv)
    loop(width // 256, turn_wo)
    gain_b[...] = jnp.broadcast_to(gain_ref[...], (128, width)).T

    gain_hi = gain_b[...].astype(BF16)
    gain_lo = (gain_b[...] - gain_hi.astype(F32)).astype(BF16)
    gains = jnp.concatenate([gain_hi, gain_lo], axis=1)

    def weigh(m):
        both = dot_nn(wqkv_t[rows_at(m, 480), :], gains) * (1.0 / width)
        gain_w[rows_at(m, 480), :] = both[:, :128] + both[:, 128:]

    CH = 160
    PIECE = 256
    pieces = width // PIECE
    chunks = width // CH

    def gain_rows(c, size):
        part = gain_b[rows_at(c, size), :]
        return jnp.concatenate([part] * (slots // 128), axis=1)

    def forward(p):
        chosen = arrival_ref[p]
        count = counts_ref[chosen]

        def turn(c, total):
            piece = x_ref[chosen, :, rows_at(c, 256)].T
            x_t[rows_at(c, 256), :] = piece
            return total + fold(piece.astype(F32))

        zero = jnp.zeros((8, slots), F32)
        total = lax.fori_loop(0, width // 256, turn, zero)
        mean = jnp.sum(total, axis=0, keepdims=True) * (1.0 / width)

        def add_sq(c, total):
            centered = x_t[rows_at(c, 320), :].astype(F32) - mean
            return total + fold(centered * centered)

        total = lax.fori_loop(0, width // 320, add_sq, zero)
        var = jnp.sum(total, axis=0, keepdims=True) * (1.0 / width)
        inv = lax.rsqrt(var + EPSILON)
        stats[0:1, :] = inv

        def norm(c):
            normed = (x_t[rows_at(c, CH), :].astype(F32) - mean) * inv
            norm_t[rows_at(c, CH), :] = normed
            hid_t[rows_at(c, CH), :] = (normed * gain_rows(c, CH)).astype(BF16)

        loop(chunks, norm)

        def pack(m):
            pk_t[rows_at(m, 480), :] = dot_nn(wqkv_t[rows_at(m, 480), :], hid_t[...]).astype(BF16)

        loop(packed // 480, pack)
        keep = lax.broadcasted_iota(jnp.int32, (slots, slots), 0) < count

        def head(h):
            q = pk_t[rows_at(h, HDIM), :]
            k = pk_t[rows_at(h + HEADS, HDIM), :]
            v = pk_t[rows_at(h + 2 * HEADS, HDIM), :]
            s = dot_nn(k.T, q) * scale
            s = jnp.where(keep, s, -1e30)
            e = jnp.exp(s - jnp.max(s, axis=0, keepdims=True))
            prob = e * (1.0 / jnp.sum(e, axis=0, keepdims=True))
            prob_f[h] = prob
            half = prob.astype(BF16)
            prob_h[h] = half
            v_n[h] = v.T
            attn_t[rows_at(h, HDIM), :] = dot_nn(v, half).astype(BF16)

        for h in range(HEADS):
            head(h)

    def take_cotangent(p, c):
        count = counts_ref[arrival_ref[p]]
        keep = (lax.broadcasted_iota(jnp.int32, (1, slots), 1) < count).astype(F32)
        piece = cot_ref[p, :, rows_at(c, PIECE)].T.astype(F32) * keep
        g_recv[p, rows_at(c, PIECE), :] = piece.astype(BF16)

    def hop(p, c):
        return pltpu.make_async_remote_copy(
            src_ref=g_send.at[p, rows_at(c, PIECE)],
            dst_ref=g_recv.at[p, rows_at(c, PIECE)],
            send_sem=send_sem.at[p, c],
            recv_sem=recv_sem.at[p, c],
            device_id={"section": below},
            device_id_type=MESH,
        )

    def backward(p):
        for c in range(pieces):

            @pl.when(sec == sections - 1)
            def _():
                take_cotangent(p, c)

            @pl.when(sec < sections - 1)
            def _():
                hop(p, c).wait_recv()

            part = dot_nn(wo_t[:, rows_at(c, PIECE)], g_recv[p, rows_at(c, PIECE), :])
            if c == 0:
                ga_acc[...] = part
            elif c < pieces - 1:
                ga_acc[...] += part
            else:
                ga_t[...] = (ga_acc[...] + part).astype(BF16)

        first = jnp.zeros((8, slots), F32)
        second = jnp.zeros((8, slots), F32)
        for h in range(HEADS):
            q = pk_t[rows_at(h, HDIM), :]
            k = pk_t[rows_at(h + HEADS, HDIM), :]
            v = pk_t[rows_at(h + 2 * HEADS, HDIM), :]
            ga = ga_t[rows_at(h, HDIM), :]
            prob = prob_f[h]
            grad_prob = dot_nn(v_n[h], ga)
            inner = jnp.sum(prob * grad_prob, axis=0, keepdims=True)
            gs = (prob * (grad_prob - inner) * scale).astype(BF16)
            grads = (dot_nn(k, gs), dot_nt(q, gs), dot_nt(ga, prob_h[h]))
            for i, (grad, own) in enumerate(zip(grads, (q, k, v))):
                at = rows_at(h + i * HEADS, HDIM)
                half = grad.astype(BF16)
                gpk_t[at, :] = half
                full = half.astype(F32)
                w = gain_w[at, :]
                first += fold(full * jnp.concatenate([w] * (slots // 128), axis=1))
                second += fold(full * own.astype(F32))
        return (
            jnp.sum(first, axis=0, keepdims=True),
            jnp.sum(second, axis=0, keepdims=True) * (1.0 / width),
        )

    def pass_down(p, first, second):
        inv = stats[0:1, :]

        def grad_hidden(c):
            at = rows_at(c, PIECE)
            gn = dot_nn(wqkv_ref[at, :], gpk_t[...]) * gain_rows(c, PIECE)
            grad_ln = inv * (gn - first - norm_t[at, :] * second)
            g_send[p, at, :] = (g_recv[p, at, :].astype(F32) + grad_ln).astype(BF16)
            hop(p, c).start()

        loop(pieces, grad_hidden)

    def weights(p):
        def qkv(n):
            acc_q[:, rows_at(n, 256)] += dot_nt(hid_t[...], gpk_t[rows_at(n, 256), :])

        loop(packed // 256, qkv)
        tail = packed // 256 * 256
        acc_q[:, tail:packed] += dot_nt(hid_t[...], gpk_t[tail:packed, :])

        def out(n):
            acc_o[:, rows_at(n, 256)] += dot_nt(g_recv[p], attn_t[rows_at(n, 256), :])

        loop(head_span // 256, out)
        tail = head_span // 256 * 256
        acc_o[:, tail:head_span] += dot_nt(g_recv[p], attn_t[tail:head_span, :])

    def clear(c):
        acc_q[rows_at(c, 64), :] = jnp.zeros((64, packed), F32)
        acc_o[rows_at(c, 64), :] = jnp.zeros((64, head_span), F32)

    forward(0)
    loop(packed // 480, weigh)

    def moment(p):
        sums = backward(p)

        @pl.when((sec == sections - 1) & (p == 0) & (core == 1))
        def _():
            pl.semaphore_wait(go_sem, 1)

        @pl.when(sec > 0)
        def _():
            pass_down(p, *sums)

        @pl.when(p == 0)
        def _():
            loop(width // 64, clear)

        weights(p)

        @pl.when((sec == sections - 1) & (p == 0) & (core == 0))
        def _():
            pl.semaphore_signal(go_sem, inc=1, device_id={"dp": twin}, device_id_type=MESH)

        @pl.when(p < micro - 1)
        def _():
            forward(p + 1)

    loop(micro, moment)

    @pl.when(sec > 0)
    def _():
        def drain(p):
            for c in range(pieces):
                hop(p, c).wait_send()

        loop(micro, drain)

    def finish(c):
        out_ref[rows_at(c, 64), 0:packed] = acc_q[rows_at(c, 64), :].astype(BF16)
        out_ref[rows_at(c, 64), packed:] = acc_o[rows_at(c, 64), :].astype(BF16)

    loop(width // 64, finish)


def run_pipeline(sections, counts, arrival, x, cotangent, gain, wqkv, wo):
    micro, slots, width = x.shape
    packed, head_span = wqkv.shape[1], wo.shape[1]
    vmem = pl.BlockSpec(memory_space=pltpu.VMEM)
    smem = pl.BlockSpec(memory_space=pltpu.SMEM)
    scratch = [
        pltpu.VMEM((packed, width), BF16),
        pltpu.VMEM((head_span, width), BF16),
        pltpu.VMEM((width, 128), F32),
        pltpu.VMEM((width, slots), BF16),
        pltpu.VMEM((width, slots), F32),
        pltpu.VMEM((width, slots), BF16),
        pltpu.VMEM((8, slots), F32),
        pltpu.VMEM((packed, slots), BF16),
        pltpu.VMEM((HEADS, slots, HDIM), BF16),
        pltpu.VMEM((HEADS, slots, slots), F32),
        pltpu.VMEM((HEADS, slots, slots), BF16),
        pltpu.VMEM((head_span, slots), BF16),
        pltpu.VMEM((head_span, slots), BF16),
        pltpu.VMEM((head_span, slots), F32),
        pltpu.VMEM((packed, slots), BF16),
        pltpu.VMEM((packed, 128), F32),
        pltpu.VMEM((width, packed), F32),
        pltpu.VMEM((width, head_span), F32),
        pltpu.VMEM((micro, width, slots), BF16),
        pltpu.VMEM((micro, width, slots), BF16),
        pltpu.SemaphoreType.DMA((micro, width // 256)),
        pltpu.SemaphoreType.DMA((micro, width // 256)),
        pltpu.SemaphoreType.REGULAR,
    ]
    return pl.pallas_call(
        functools.partial(pipeline_kernel, sections),
        out_shape=jax.ShapeDtypeStruct((width, packed + head_span), BF16),
        in_specs=[smem, smem, vmem, vmem, vmem, vmem, vmem],
        out_specs=vmem,
        scratch_shapes=scratch,
        compiler_params=pltpu.CompilerParams(
            collective_id=0, has_side_effects=True, vmem_limit_bytes=64 * 1024 * 1024 - 65536
        ),
        name="pipeline",
    )(counts, arrival, x, cotangent, gain, wqkv, wo)


def per_device(activations, cotangent, counts, arrival, norm_gain, qkv_weight, out_weight):
    sections = lax.axis_size("section")
    packed = qkv_weight.shape[2]
    both = run_pipeline(
        sections,
        counts[:, 0],
        arrival,
        activations[0],
        cotangent,
        norm_gain,
        qkv_weight[0],
        out_weight[0],
    )
    share = lax.psum_scatter(both, "dp", scatter_dimension=0, tiled=True).astype(F32)
    return (share[None, :, :packed], share[None, :, packed:])


def solution(mesh):
    placed = (
        P("section", None, "dp", None),
        P(None, "dp", None),
        P(None, "dp"),
        P(),
        P("section", None),
        P("section", None, None),
        P("section", None, None),
    )
    return jax.shard_map(
        per_device,
        mesh=mesh,
        in_specs=placed,
        out_specs=(P("section", "dp", None), P("section", "dp", None)),
        check_vma=False,
    )
```

```python
import functools

import jax
import jax.numpy as jnp
from jax import lax
from jax.experimental import pallas as pl
from jax.experimental.pallas import tpu as pltpu
from jax.sharding import PartitionSpec as P

HDIM = 80
HEADS = 8
EPSILON = 1e-06
MESH = pl.DeviceIdType.MESH
TILE = 256
TX = 6
F32 = jnp.float32
BF16 = jnp.bfloat16


def dot_nn(a, b):
    return lax.dot_general(a, b, (((1,), (0,)), ((), ())), preferred_element_type=F32)


def dot_nt(a, b):
    return lax.dot_general(a, b, (((1,), (1,)), ((), ())), preferred_element_type=F32)


def fold(a):
    return jnp.sum(a.reshape(a.shape[0] // 8, 8, a.shape[1]), axis=0)


def loop(count, body):
    def step(i, carry):
        body(i)
        return carry

    lax.fori_loop(0, count, step, 0)


def rows_at(i, size):
    if isinstance(i, int):
        return pl.ds(i * size, size)
    return pl.ds(pl.multiple_of(i * size, size), size)


def pipeline_kernel(
    sections,
    counts_ref,
    arrival_ref,
    x_ref,
    cot_ref,
    gain_ref,
    wqkv_ref,
    wo_ref,
    qkv_out,
    out_out,
    wqkv_t,
    wo_t,
    gain_b,
    x_t,
    norm_t,
    hid_t,
    stats,
    pk_t,
    v_n,
    prob_f,
    prob_h,
    attn_t,
    ga_t,
    ga_acc,
    gpk_t,
    gain_w,
    acc,
    g_recv,
    g_send,
    send_sem,
    recv_sem,
    go_sem,
    stage,
    got_a,
    got_y1,
    got_x1,
    got_x2,
    got_y2,
    got_y3,
    got_x3,
    send_x3,
    rs_send,
    rs_recv,
):
    micro, slots, width = x_ref.shape
    head_span = wo_ref.shape[1]
    packed = wqkv_ref.shape[1]
    scale = HDIM**-0.5
    sec = lax.axis_index("section")
    below = lax.rem(sec + sections - 1, sections)
    above = lax.rem(sec + 1, sections)
    lane = lax.axis_index("dp")
    core = lax.rem(lane, 2)
    twin = lane + 1 - 2 * core
    row = lax.rem(lane // 2, 2)
    col = lane // 4
    cols = stage.shape[1]
    right, left, far = (lax.rem(col + step, cols) for step in (1, cols - 1, 2))
    rest = row * 2 + core
    to_right = right * 4 + rest
    to_left = left * 4 + rest
    to_row = col * 4 + (1 - row) * 2 + core
    barrier = pltpu.get_barrier_semaphore()
    for other in (below, above):
        pl.semaphore_signal(barrier, inc=1, device_id={"section": other}, device_id_type=MESH)
    for other in (twin, to_right, to_left, to_row):
        pl.semaphore_signal(barrier, inc=1, device_id={"dp": other}, device_id_type=MESH)
    pl.semaphore_wait(barrier, 6)

    def turn_wo(c):
        wo_t[:, rows_at(c, 256)] = wo_ref[rows_at(c, 256), :].T

    def turn_wqkv(c):
        wqkv_t[:, rows_at(c, 256)] = wqkv_ref[rows_at(c, 256), :].T

    loop(width // 256, turn_wqkv)
    loop(width // 256, turn_wo)
    gain_b[...] = jnp.broadcast_to(gain_ref[...], (128, width)).T

    gain_hi = gain_b[...].astype(BF16)
    gain_lo = (gain_b[...] - gain_hi.astype(F32)).astype(BF16)
    gains = jnp.concatenate([gain_hi, gain_lo], axis=1)

    def weigh(m):
        both = dot_nn(wqkv_t[rows_at(m, 480), :], gains) * (1.0 / width)
        gain_w[rows_at(m, 480), :] = both[:, :128] + both[:, 128:]

    CH = 160
    PIECE = 256
    pieces = width // PIECE
    tiles = acc.shape[0]
    whole = packed // TILE
    edge = TILE - (packed - whole * TILE)
    chunks = width // CH

    def gain_rows(c, size):
        part = gain_b[rows_at(c, size), :]
        return jnp.concatenate([part] * (slots // 128), axis=1)

    def forward(p):
        chosen = arrival_ref[p]
        count = counts_ref[chosen]

        def turn(c, total):
            piece = x_ref[chosen, :, rows_at(c, 256)].T
            x_t[rows_at(c, 256), :] = piece
            return total + fold(piece.astype(F32))

        zero = jnp.zeros((8, slots), F32)
        total = lax.fori_loop(0, width // 256, turn, zero)
        mean = jnp.sum(total, axis=0, keepdims=True) * (1.0 / width)

        def add_sq(c, total):
            centered = x_t[rows_at(c, 320), :].astype(F32) - mean
            return total + fold(centered * centered)

        total = lax.fori_loop(0, width // 320, add_sq, zero)
        var = jnp.sum(total, axis=0, keepdims=True) * (1.0 / width)
        inv = lax.rsqrt(var + EPSILON)
        stats[0:1, :] = inv

        def norm(c):
            normed = (x_t[rows_at(c, CH), :].astype(F32) - mean) * inv
            norm_t[rows_at(c, CH), :] = normed
            hid_t[rows_at(c, CH), :] = (normed * gain_rows(c, CH)).astype(BF16)

        loop(chunks, norm)

        def pack(m):
            pk_t[rows_at(m, 480), :] = dot_nn(wqkv_t[rows_at(m, 480), :], hid_t[...]).astype(BF16)

        loop(packed // 480, pack)
        keep = lax.broadcasted_iota(jnp.int32, (slots, slots), 0) < count

        def head(h):
            q = pk_t[rows_at(h, HDIM), :]
            k = pk_t[rows_at(h + HEADS, HDIM), :]
            v = pk_t[rows_at(h + 2 * HEADS, HDIM), :]
            s = dot_nn(k.T, q) * scale
            s = jnp.where(keep, s, -1e30)
            e = jnp.exp(s - jnp.max(s, axis=0, keepdims=True))
            prob = e * (1.0 / jnp.sum(e, axis=0, keepdims=True))
            prob_f[h] = prob
            half = prob.astype(BF16)
            prob_h[h] = half
            v_n[h] = v.T
            attn_t[rows_at(h, HDIM), :] = dot_nn(v, half).astype(BF16)

        for h in range(HEADS):
            head(h)

    def take_cotangent(p, c):
        count = counts_ref[arrival_ref[p]]
        keep = (lax.broadcasted_iota(jnp.int32, (1, slots), 1) < count).astype(F32)
        piece = cot_ref[p, :, rows_at(c, PIECE)].T.astype(F32) * keep
        g_recv[p, rows_at(c, PIECE), :] = piece.astype(BF16)

    def hop(p, c):
        return pltpu.make_async_remote_copy(
            src_ref=g_send.at[p, rows_at(c, PIECE)],
            dst_ref=g_recv.at[p, rows_at(c, PIECE)],
            send_sem=send_sem.at[p, c],
            recv_sem=recv_sem.at[p, c],
            device_id={"section": below},
            device_id_type=MESH,
        )

    def backward(p):
        for c in range(pieces):

            @pl.when(sec == sections - 1)
            def _():
                take_cotangent(p, c)

            @pl.when(sec < sections - 1)
            def _():
                hop(p, c).wait_recv()

            part = dot_nn(wo_t[:, rows_at(c, PIECE)], g_recv[p, rows_at(c, PIECE), :])
            if c == 0:
                ga_acc[...] = part
            elif c < pieces - 1:
                ga_acc[...] += part
            else:
                ga_t[...] = (ga_acc[...] + part).astype(BF16)

        first = jnp.zeros((8, slots), F32)
        second = jnp.zeros((8, slots), F32)
        for h in range(HEADS):
            q = pk_t[rows_at(h, HDIM), :]
            k = pk_t[rows_at(h + HEADS, HDIM), :]
            v = pk_t[rows_at(h + 2 * HEADS, HDIM), :]
            ga = ga_t[rows_at(h, HDIM), :]
            prob = prob_f[h]
            grad_prob = dot_nn(v_n[h], ga)
            inner = jnp.sum(prob * grad_prob, axis=0, keepdims=True)
            gs = (prob * (grad_prob - inner) * scale).astype(BF16)
            grads = (dot_nn(k, gs), dot_nt(q, gs), dot_nt(ga, prob_h[h]))
            for i, (grad, own) in enumerate(zip(grads, (q, k, v))):
                at = rows_at(h + i * HEADS, HDIM)
                half = grad.astype(BF16)
                gpk_t[at, :] = half
                full = half.astype(F32)
                w = gain_w[at, :]
                first += fold(full * jnp.concatenate([w] * (slots // 128), axis=1))
                second += fold(full * own.astype(F32))
        return (
            jnp.sum(first, axis=0, keepdims=True),
            jnp.sum(second, axis=0, keepdims=True) * (1.0 / width),
        )

    def pass_down(p, first, second):
        inv = stats[0:1, :]

        def grad_hidden(c):
            at = rows_at(c, PIECE)
            gn = dot_nn(wqkv_ref[at, :], gpk_t[...]) * gain_rows(c, PIECE)
            grad_ln = inv * (gn - first - norm_t[at, :] * second)
            g_send[p, at, :] = (g_recv[p, at, :].astype(F32) + grad_ln).astype(BF16)
            hop(p, c).start()

        loop(pieces, grad_hidden)

    def tile(p, n):
        if isinstance(n, int) and n == whole:
            half = dot_nt(hid_t[...], gpk_t[n * TILE : packed, :])
            return jnp.concatenate([half, dot_nt(g_recv[p], attn_t[0:edge, :])], axis=1)
        if isinstance(n, int) and n > whole:
            start = edge + (n - whole - 1) * TILE
            return dot_nt(g_recv[p], attn_t[start : start + TILE, :])
        return dot_nt(hid_t[...], gpk_t[rows_at(n, TILE), :])

    def weights(p):
        def qkv(n):
            acc[n] += tile(p, n)

        loop(whole, qkv)
        for n in range(whole, tiles):
            acc[n] += tile(p, n)

    def give_twin(n):
        return send(stage.at[n, :, :, 1 - core], got_a.at[n], n, twin)

    def send(src, dst, i, lane_to):
        return pltpu.make_async_remote_copy(
            src_ref=src,
            dst_ref=dst,
            send_sem=rs_send.at[i],
            recv_sem=rs_recv.at[i],
            device_id={"dp": lane_to},
            device_id_type=MESH,
        )

    def last_weights(p):
        def put(n):
            total = (acc[n] + tile(p, n)).astype(BF16)
            stage[n] = total.reshape(stage.shape[1:])
            give_twin(n).start()

        for n in range(whole, tiles):
            put(n)

        def qkv(i):
            put(whole - 1 - i)

        loop(whole, qkv)

    def join(at, other):
        stage[at] = (stage[at].astype(F32) + other.astype(F32)).astype(BF16)

    def reduce_out():
        nx, ny = TX, tiles - TX
        hx, hy = nx // 2, ny // 2
        xa, xb = pl.ds(0, hx), pl.ds(hx, nx - hx)
        ya, yb = pl.ds(nx, hy), pl.ds(nx + hy, ny - hy)
        base = tiles
        y1 = [
            send(stage.at[nx + i, :, 1 - row, core], got_y1.at[i], base + i, to_row)
            for i in range(ny)
        ]
        base += ny
        x1 = (
            send(stage.at[xa, far, :, core], got_x1.at[0, 0:hx], base, to_right),
            send(stage.at[xb, far, :, core], got_x1.at[1, 0 : nx - hx], base + 1, to_left),
        )
        x2a = (
            send(stage.at[xb, right, :, core], got_x2.at[0, hx:nx], base + 2, to_right),
            send(stage.at[xa, left, :, core], got_x2.at[1, 0:hx], base + 3, to_left),
        )
        x2b = (
            send(stage.at[xa, right, :, core], got_x2.at[0, 0:hx], base + 4, to_right),
            send(stage.at[xb, left, :, core], got_x2.at[1, hx:nx], base + 5, to_left),
        )
        y2 = (
            send(stage.at[ya, far, row, core], got_y2.at[0, 0:hy], base + 6, to_right),
            send(stage.at[yb, far, row, core], got_y2.at[1, 0 : ny - hy], base + 7, to_left),
        )
        y3a = (
            send(stage.at[yb, right, row, core], got_y3.at[0, hy:ny], base + 8, to_right),
            send(stage.at[ya, left, row, core], got_y3.at[1, 0:hy], base + 9, to_left),
        )
        y3b = (
            send(stage.at[ya, right, row, core], got_y3.at[0, 0:hy], base + 10, to_right),
            send(stage.at[yb, left, row, core], got_y3.at[1, hy:ny], base + 11, to_left),
        )
        x3 = send(send_x3, got_x3, base + 12, to_row)

        def meet(n):
            give_twin(n).wait_recv()
            for c in range(cols):
                join((n, c, slice(None), core), got_a[n, c])

        for i in reversed(range(ny)):
            meet(nx + i)
            y1[i].start()

        def meet_x(i):
            meet(nx - 1 - i)

        loop(nx, meet_x)
        for copy in x1 + x2a:
            copy.start()
        for i in range(ny):
            y1[i].wait_recv()
            for c in range(cols):
                join((nx + i, c, row, core), got_y1[i, c])
        x1[0].wait_recv()
        for i in range(hx):
            join((i, right, slice(None), core), got_x1[0, i])
        x2b[0].start()
        x1[1].wait_recv()
        for i in range(nx - hx):
            join((hx + i, left, slice(None), core), got_x1[1, i])
        x2b[1].start()
        for copy in y2 + y3a:
            copy.start()
        y2[0].wait_recv()
        for i in range(hy):
            join((nx + i, right, row, core), got_y2[0, i])
        y3b[0].start()
        y2[1].wait_recv()
        for i in range(ny - hy):
            join((nx + hy + i, left, row, core), got_y2[1, i])
        y3b[1].start()

        def across(n, r):
            total = stage[n, col, r, core].astype(F32) + got_x2[0, n, r].astype(F32)
            return total + got_x2[1, n, r].astype(F32)

        for copy in x2a + x2b:
            copy.wait_recv()
        for n in range(nx):
            send_x3[n] = across(n, 1 - row).astype(BF16)
        x3.start()

        def emit(n, value):
            if n < whole:
                qkv_out[:, n * TILE : (n + 1) * TILE] = value
            elif n == whole:
                qkv_out[:, n * TILE : packed] = value[:, : TILE - edge]
                out_out[:, 0:edge] = value[:, TILE - edge :]
            else:
                start = edge + (n - whole - 1) * TILE
                out_out[:, start : start + TILE] = value

        for copy in y3a + y3b:
            copy.wait_recv()
        for i in range(ny):
            total = stage[nx + i, col, row, core].astype(F32) + got_y3[0, i].astype(F32)
            emit(nx + i, total + got_y3[1, i].astype(F32))
        x3.wait_recv()
        for n in range(nx):
            emit(n, across(n, row) + got_x3[n].astype(F32))
        for copy in tuple(y1) + x1 + x2a + x2b + y2 + y3a + y3b + (x3,):
            copy.wait_send()

        def given(n):
            give_twin(n).wait_send()

        loop(tiles, given)

    def clear(c):
        acc[:, rows_at(c, 32), :] = jnp.zeros((tiles, 32, TILE), F32)

    forward(0)
    loop(packed // 480, weigh)

    def moment(p):
        sums = backward(p)

        @pl.when((sec == sections - 1) & (p == 0) & (core == 1))
        def _():
            pl.semaphore_wait(go_sem, 1)

        @pl.when(sec > 0)
        def _():
            pass_down(p, *sums)

        @pl.when(p == 0)
        def _():
            loop(width // 32, clear)

        @pl.when(p < micro - 1)
        def _():
            weights(p)

        @pl.when(p == micro - 1)
        def _():
            last_weights(p)

        @pl.when((sec == sections - 1) & (p == 0) & (core == 0))
        def _():
            pl.semaphore_signal(go_sem, inc=1, device_id={"dp": twin}, device_id_type=MESH)

        @pl.when(p < micro - 1)
        def _():
            forward(p + 1)

    loop(micro, moment)
    reduce_out()

    @pl.when(sec > 0)
    def _():
        def drain(p):
            for c in range(pieces):
                hop(p, c).wait_send()

        loop(micro, drain)


def run_pipeline(sections, lanes, counts, arrival, x, cotangent, gain, wqkv, wo):
    micro, slots, width = x.shape
    packed, head_span = wqkv.shape[1], wo.shape[1]
    tiles, cols, share = (packed + head_span) // TILE, lanes // 4, width // lanes
    vmem = pl.BlockSpec(memory_space=pltpu.VMEM)
    smem = pl.BlockSpec(memory_space=pltpu.SMEM)
    scratch = [
        pltpu.VMEM((packed, width), BF16),
        pltpu.VMEM((head_span, width), BF16),
        pltpu.VMEM((width, 128), F32),
        pltpu.VMEM((width, slots), BF16),
        pltpu.VMEM((width, slots), F32),
        pltpu.VMEM((width, slots), BF16),
        pltpu.VMEM((8, slots), F32),
        pltpu.VMEM((packed, slots), BF16),
        pltpu.VMEM((HEADS, slots, HDIM), BF16),
        pltpu.VMEM((HEADS, slots, slots), F32),
        pltpu.VMEM((HEADS, slots, slots), BF16),
        pltpu.VMEM((head_span, slots), BF16),
        pltpu.VMEM((head_span, slots), BF16),
        pltpu.VMEM((head_span, slots), F32),
        pltpu.VMEM((packed, slots), BF16),
        pltpu.VMEM((packed, 128), F32),
        pltpu.VMEM((tiles, width, TILE), F32),
        pltpu.VMEM((micro, width, slots), BF16),
        pltpu.VMEM((micro, width, slots), BF16),
        pltpu.SemaphoreType.DMA((micro, width // 256)),
        pltpu.SemaphoreType.DMA((micro, width // 256)),
        pltpu.SemaphoreType.REGULAR,
        pltpu.VMEM((tiles, cols, 2, 2, share, TILE), BF16),
        pltpu.VMEM((tiles, cols, 2, share, TILE), BF16),
        pltpu.VMEM((tiles - TX, cols, share, TILE), BF16),
        pltpu.VMEM((2, TX - TX // 2, 2, share, TILE), BF16),
        pltpu.VMEM((2, TX, 2, share, TILE), BF16),
        pltpu.VMEM((2, tiles - TX - (tiles - TX) // 2, share, TILE), BF16),
        pltpu.VMEM((2, tiles - TX, share, TILE), BF16),
        pltpu.VMEM((TX, share, TILE), BF16),
        pltpu.VMEM((TX, share, TILE), BF16),
        pltpu.SemaphoreType.DMA((tiles + tiles - TX + 13,)),
        pltpu.SemaphoreType.DMA((tiles + tiles - TX + 13,)),
    ]
    return pl.pallas_call(
        functools.partial(pipeline_kernel, sections),
        out_shape=(
            jax.ShapeDtypeStruct((share, packed), F32),
            jax.ShapeDtypeStruct((share, head_span), F32),
        ),
        in_specs=[smem, smem, vmem, vmem, vmem, vmem, vmem],
        out_specs=(vmem, vmem),
        scratch_shapes=scratch,
        compiler_params=pltpu.CompilerParams(
            collective_id=0, has_side_effects=True, vmem_limit_bytes=64 * 1024 * 1024 - 65536
        ),
        name="pipeline",
    )(counts, arrival, x, cotangent, gain, wqkv, wo)


def per_device(activations, cotangent, counts, arrival, norm_gain, qkv_weight, out_weight):
    sections = lax.axis_size("section")
    qkv_share, out_share = run_pipeline(
        sections,
        lax.axis_size("dp"),
        counts[:, 0],
        arrival,
        activations[0],
        cotangent,
        norm_gain,
        qkv_weight[0],
        out_weight[0],
    )
    return (qkv_share[None], out_share[None])


def solution(mesh):
    placed = (
        P("section", None, "dp", None),
        P(None, "dp", None),
        P(None, "dp"),
        P(),
        P("section", None),
        P("section", None, None),
        P("section", None, None),
    )
    return jax.shard_map(
        per_device,
        mesh=mesh,
        in_specs=placed,
        out_specs=(P("section", "dp", None), P("section", "dp", None)),
        check_vma=False,
    )
```

```python
import functools

import jax
import jax.numpy as jnp
from jax import lax
from jax.experimental import pallas as pl
from jax.experimental.pallas import tpu as pltpu
from jax.sharding import PartitionSpec as P

HDIM = 80
HEADS = 8
EPSILON = 1e-06
MESH = pl.DeviceIdType.MESH
TILE = 256
PIECE = 256
TX = 6
TURN = 2
F32 = jnp.float32
BF16 = jnp.bfloat16


def dot_nn(a, b):
    return lax.dot_general(a, b, (((1,), (0,)), ((), ())), preferred_element_type=F32)


def dot_nt(a, b):
    return lax.dot_general(a, b, (((1,), (1,)), ((), ())), preferred_element_type=F32)


def fold(a):
    return jnp.sum(a.reshape(a.shape[0] // 8, 8, a.shape[1]), axis=0)


def loop(count, body):
    def step(i, carry):
        body(i)
        return carry

    lax.fori_loop(0, count, step, 0)


def rows_at(i, size):
    if isinstance(i, int):
        return pl.ds(i * size, size)
    return pl.ds(pl.multiple_of(i * size, size), size)


def pipeline_kernel(
    sections,
    counts_ref,
    arrival_ref,
    x_hbm,
    cot_hbm,
    gain_ref,
    wqkv_hbm,
    wo_hbm,
    qkv_out,
    out_out,
    x_ref,
    cot_ref,
    wqkv_ref,
    wqkv_t,
    wo_t,
    gain_b,
    gain_w,
    x_t,
    hid_t,
    stats,
    pk_t,
    prob_h,
    attn_t,
    ga_t,
    ga_acc,
    gpk_t,
    acc,
    g_recv,
    g_send,
    send_sem,
    recv_sem,
    go_sem,
    load_sem,
    stage,
    got_a,
    got_y1,
    got_x1,
    got_x2,
    got_y2,
    got_y3,
    got_x3,
    send_x3,
    rs_send,
    rs_recv,
):
    micro, slots, width = x_ref.shape
    head_span = wo_hbm.shape[1]
    packed = wqkv_ref.shape[1]
    scale = HDIM**-0.5
    pieces = width // PIECE
    tiles = acc.shape[0]
    whole = packed // TILE
    edge = TILE - (packed - whole * TILE)
    sec = lax.axis_index("section")
    below = lax.rem(sec + sections - 1, sections)
    above = lax.rem(sec + 1, sections)
    lane = lax.axis_index("dp")
    core = lax.rem(lane, 2)
    twin = lane + 1 - 2 * core
    row = lax.rem(lane // 2, 2)
    col = lane // 4
    cols = stage.shape[1]
    right, left, far = (lax.rem(col + step, cols) for step in (1, cols - 1, 2))
    rest = row * 2 + core
    to_right = right * 4 + rest
    to_left = left * 4 + rest
    to_row = col * 4 + (1 - row) * 2 + core
    top = sec == sections - 1

    def load(src, dst, i):
        return pltpu.make_async_copy(src, dst, load_sem.at[i])

    def load_cot(p):
        return load(cot_hbm.at[p], cot_ref, 0)

    load_x = load(x_hbm, x_ref, 1)
    load_w = [
        load(wqkv_hbm.at[rows_at(c, PIECE)], wqkv_ref.at[rows_at(c, PIECE)], 2 + c)
        for c in range(pieces)
    ]
    wo_parts = [(at, min(PIECE, head_span - at)) for at in range(0, head_span, PIECE)]
    load_wo = [
        load(
            wo_hbm.at[:, pl.ds(at, size)],
            hid_t.at[1 + i, :, pl.ds(0, size)],
            2 + pieces + i,
        )
        for i, (at, size) in enumerate(wo_parts)
    ]
    load_x.start()
    for copy in load_w + load_wo:
        copy.start()

    @pl.when(top)
    def _():
        load_cot(0).start()

    barrier = pltpu.get_barrier_semaphore()
    for other in (below, above):
        pl.semaphore_signal(barrier, inc=1, device_id={"section": other}, device_id_type=MESH)
    for other in (twin, to_right, to_left, to_row):
        pl.semaphore_signal(barrier, inc=1, device_id={"dp": other}, device_id_type=MESH)
    pl.semaphore_wait(barrier, 6)
    gain_b[...] = jnp.broadcast_to(gain_ref[...], (128, width)).T
    load_x.wait()

    def turn_weights():
        for c in range(pieces):
            load_w[c].wait()
            wqkv_t[:, rows_at(c, PIECE)] = wqkv_ref[rows_at(c, PIECE), :].T
        for i, (at, size) in enumerate(wo_parts):
            load_wo[i].wait()
            wo_t[at : at + size, :] = hid_t[1 + i, :, 0:size].T
        gain_hi = gain_b[...].astype(BF16)
        gain_lo = (gain_b[...] - gain_hi.astype(F32)).astype(BF16)
        gains = jnp.concatenate([gain_hi, gain_lo], axis=1)

        def weigh(m):
            both = dot_nn(wqkv_t[rows_at(m, 480), :], gains) * (1.0 / width)
            gain_w[rows_at(m, 480), :] = both[:, :128] + both[:, 128:]

        loop(packed // 480, weigh)

    CH = 160
    chunks = width // CH

    def gain_rows(c, size):
        part = gain_b[rows_at(c, size), :]
        return jnp.concatenate([part] * (slots // 128), axis=1)

    def normalize(p):
        chosen = arrival_ref[p]

        def turn(c, total):
            piece = x_ref[chosen, :, rows_at(c, PIECE)].T
            x_t[p, rows_at(c, PIECE), :] = piece
            return total + fold(piece.astype(F32))

        zero = jnp.zeros((8, slots), F32)
        total = lax.fori_loop(0, pieces, turn, zero)
        mean = jnp.sum(total, axis=0, keepdims=True) * (1.0 / width)

        def add_sq(c, total):
            centered = x_t[p, rows_at(c, 320), :].astype(F32) - mean
            return total + fold(centered * centered)

        total = lax.fori_loop(0, width // 320, add_sq, zero)
        var = jnp.sum(total, axis=0, keepdims=True) * (1.0 / width)
        inv = lax.rsqrt(var + EPSILON)
        stats[p, 0:1, :] = inv
        stats[p, 1:2, :] = mean

    def attend(p):
        count = counts_ref[arrival_ref[p]]
        inv = stats[p, 0:1, :]
        mean = stats[p, 1:2, :]

        def norm(c):
            normed = (x_t[p, rows_at(c, CH), :].astype(F32) - mean) * inv
            hid_t[p, rows_at(c, CH), :] = (normed * gain_rows(c, CH)).astype(BF16)

        loop(chunks, norm)

        def pack(m):
            part = dot_nn(wqkv_t[rows_at(m, 480), :], hid_t[p])
            pk_t[p, rows_at(m, 480), :] = part.astype(BF16)

        loop(packed // 480, pack)
        keep = lax.broadcasted_iota(jnp.int32, (slots, slots), 0) < count
        for h in range(HEADS):
            q = pk_t[p, rows_at(h, HDIM), :]
            k = pk_t[p, rows_at(h + HEADS, HDIM), :]
            v = pk_t[p, rows_at(h + 2 * HEADS, HDIM), :]
            s = jnp.where(keep, dot_nn(k.T, q) * scale, -1e30)
            e = jnp.exp(s - jnp.max(s, axis=0, keepdims=True))
            half = (e * (1.0 / jnp.sum(e, axis=0, keepdims=True))).astype(BF16)
            prob_h[p, h] = half
            attn_t[p, rows_at(h, HDIM), :] = dot_nn(v, half).astype(BF16)

    def take_cotangent(p, c):
        count = counts_ref[arrival_ref[p]]
        keep = (lax.broadcasted_iota(jnp.int32, (1, slots), 1) < count).astype(F32)
        piece = cot_ref[:, rows_at(c, PIECE)].T.astype(F32) * keep
        g_recv[p, rows_at(c, PIECE), :] = piece.astype(BF16)

    def hop(p, c):
        return pltpu.make_async_remote_copy(
            src_ref=g_send.at[lax.rem(p, 2), rows_at(c, PIECE)],
            dst_ref=g_recv.at[p, rows_at(c, PIECE)],
            send_sem=send_sem.at[p, c],
            recv_sem=recv_sem.at[p, c],
            device_id={"section": below},
            device_id_type=MESH,
        )

    def backward(p):
        @pl.when(top)
        def _():
            load_cot(p).wait()

        for c in range(pieces):

            @pl.when(top)
            def _():
                take_cotangent(p, c)

            @pl.when(jnp.logical_not(top))
            def _():
                hop(p, c).wait_recv()

            part = dot_nn(wo_t[:, rows_at(c, PIECE)], g_recv[p, rows_at(c, PIECE), :])
            if c == 0:
                ga_acc[...] = part
            elif c < pieces - 1:
                ga_acc[...] += part
            else:
                ga_t[...] = (ga_acc[...] + part).astype(BF16)

        @pl.when(top & (p < micro - 1))
        def _():
            load_cot(p + 1).start()

        first = jnp.zeros((8, slots), F32)
        second = jnp.zeros((8, slots), F32)
        for h in range(HEADS):
            q = pk_t[p, rows_at(h, HDIM), :]
            k = pk_t[p, rows_at(h + HEADS, HDIM), :]
            v = pk_t[p, rows_at(h + 2 * HEADS, HDIM), :]
            ga = ga_t[rows_at(h, HDIM), :]
            half = prob_h[p, h]
            prob = half.astype(F32)
            grad_prob = dot_nn(v.T, ga)
            inner = jnp.sum(prob * grad_prob, axis=0, keepdims=True)
            gs = (prob * (grad_prob - inner) * scale).astype(BF16)
            grads = (dot_nn(k, gs), dot_nt(q, gs), dot_nt(ga, half))
            for i, (grad, own) in enumerate(zip(grads, (q, k, v))):
                at = rows_at(h + i * HEADS, HDIM)
                rounded = grad.astype(BF16)
                gpk_t[at, :] = rounded
                full = rounded.astype(F32)
                w = gain_w[at, :]
                first += fold(full * jnp.concatenate([w] * (slots // 128), axis=1))
                second += fold(full * own.astype(F32))
        return (
            jnp.sum(first, axis=0, keepdims=True),
            jnp.sum(second, axis=0, keepdims=True) * (1.0 / width),
        )

    def pass_down(p, first, second):
        inv = stats[p, 0:1, :]
        mean = stats[p, 1:2, :]

        @pl.when(p >= 2)
        def _():
            for c in range(pieces):
                if c != TURN:
                    hop(p - 2, c).wait_send()

        def grad_hidden(c):
            at = rows_at(c, PIECE)
            gn = dot_nn(wqkv_ref[at, :], gpk_t[...]) * gain_rows(c, PIECE)
            normed = (x_t[p, at, :].astype(F32) - mean) * inv
            grad_ln = inv * (gn - first - normed * second)
            g_send[lax.rem(p, 2), at, :] = (g_recv[p, at, :].astype(F32) + grad_ln).astype(BF16)
            hop(p, c).start()

        loop(pieces, grad_hidden)

    def tile(p, n):
        if isinstance(n, int) and n == whole:
            half = dot_nt(hid_t[p], gpk_t[n * TILE : packed, :])
            return jnp.concatenate([half, dot_nt(g_recv[p], attn_t[p, 0:edge, :])], axis=1)
        if isinstance(n, int) and n > whole:
            start = edge + (n - whole - 1) * TILE
            return dot_nt(g_recv[p], attn_t[p, start : start + TILE, :])
        return dot_nt(hid_t[p], gpk_t[rows_at(n, TILE), :])

    def weights(p):
        def qkv(n):
            acc[n] += tile(p, n)

        loop(whole, qkv)
        for n in range(whole, tiles):
            acc[n] += tile(p, n)

    def give_twin(n):
        return send(stage.at[n, :, :, 1 - core], got_a.at[n], n, twin)

    def send(src, dst, i, lane_to):
        return pltpu.make_async_remote_copy(
            src_ref=src,
            dst_ref=dst,
            send_sem=rs_send.at[i],
            recv_sem=rs_recv.at[i],
            device_id={"dp": lane_to},
            device_id_type=MESH,
        )

    def last_weights(p):
        def put(n):
            total = (acc[n] + tile(p, n)).astype(BF16)
            stage[n] = total.reshape(stage.shape[1:])
            give_twin(n).start()

        for n in range(whole, tiles):
            put(n)

        def qkv(i):
            put(whole - 1 - i)

        loop(whole, qkv)

    def join(at, other):
        stage[at] = (stage[at].astype(F32) + other.astype(F32)).astype(BF16)

    def reduce_out():
        nx, ny = TX, tiles - TX
        hx, hy = nx // 2, ny // 2
        xa, xb = pl.ds(0, hx), pl.ds(hx, nx - hx)
        ya, yb = pl.ds(nx, hy), pl.ds(nx + hy, ny - hy)
        base = tiles
        y1 = [
            send(stage.at[nx + i, :, 1 - row, core], got_y1.at[i], base + i, to_row)
            for i in range(ny)
        ]
        base += ny
        x1 = (
            send(stage.at[xa, far, :, core], got_x1.at[0, 0:hx], base, to_right),
            send(stage.at[xb, far, :, core], got_x1.at[1, 0 : nx - hx], base + 1, to_left),
        )
        x2a = (
            send(stage.at[xb, right, :, core], got_x2.at[0, hx:nx], base + 2, to_right),
            send(stage.at[xa, left, :, core], got_x2.at[1, 0:hx], base + 3, to_left),
        )
        x2b = (
            send(stage.at[xa, right, :, core], got_x2.at[0, 0:hx], base + 4, to_right),
            send(stage.at[xb, left, :, core], got_x2.at[1, hx:nx], base + 5, to_left),
        )
        y2 = (
            send(stage.at[ya, far, row, core], got_y2.at[0, 0:hy], base + 6, to_right),
            send(stage.at[yb, far, row, core], got_y2.at[1, 0 : ny - hy], base + 7, to_left),
        )
        y3a = (
            send(stage.at[yb, right, row, core], got_y3.at[0, hy:ny], base + 8, to_right),
            send(stage.at[ya, left, row, core], got_y3.at[1, 0:hy], base + 9, to_left),
        )
        y3b = (
            send(stage.at[ya, right, row, core], got_y3.at[0, 0:hy], base + 10, to_right),
            send(stage.at[yb, left, row, core], got_y3.at[1, hy:ny], base + 11, to_left),
        )
        x3 = send(send_x3, got_x3, base + 12, to_row)

        def meet(n):
            give_twin(n).wait_recv()
            for c in range(cols):
                join((n, c, slice(None), core), got_a[n, c])

        for i in reversed(range(ny)):
            meet(nx + i)
            y1[i].start()

        def meet_x(i):
            meet(nx - 1 - i)

        loop(nx, meet_x)
        for copy in x1 + x2a:
            copy.start()
        for i in range(ny):
            y1[i].wait_recv()
            for c in range(cols):
                join((nx + i, c, row, core), got_y1[i, c])
        x1[0].wait_recv()
        for i in range(hx):
            join((i, right, slice(None), core), got_x1[0, i])
        x2b[0].start()
        x1[1].wait_recv()
        for i in range(nx - hx):
            join((hx + i, left, slice(None), core), got_x1[1, i])
        x2b[1].start()
        for copy in y2 + y3a:
            copy.start()
        y2[0].wait_recv()
        for i in range(hy):
            join((nx + i, right, row, core), got_y2[0, i])
        y3b[0].start()
        y2[1].wait_recv()
        for i in range(ny - hy):
            join((nx + hy + i, left, row, core), got_y2[1, i])
        y3b[1].start()

        def across(n, r):
            total = stage[n, col, r, core].astype(F32) + got_x2[0, n, r].astype(F32)
            return total + got_x2[1, n, r].astype(F32)

        for copy in x2a + x2b:
            copy.wait_recv()
        for n in range(nx):
            send_x3[n] = across(n, 1 - row).astype(BF16)
        x3.start()

        def emit(n, value):
            if n < whole:
                qkv_out[:, n * TILE : (n + 1) * TILE] = value
            elif n == whole:
                qkv_out[:, n * TILE : packed] = value[:, : TILE - edge]
                out_out[:, 0:edge] = value[:, TILE - edge :]
            else:
                start = edge + (n - whole - 1) * TILE
                out_out[:, start : start + TILE] = value

        for copy in y3a + y3b:
            copy.wait_recv()
        for i in range(ny):
            total = stage[nx + i, col, row, core].astype(F32) + got_y3[0, i].astype(F32)
            emit(nx + i, total + got_y3[1, i].astype(F32))
        x3.wait_recv()
        for n in range(nx):
            emit(n, across(n, row) + got_x3[n].astype(F32))
        for copy in tuple(y1) + x1 + x2a + x2b + y2 + y3a + y3b + (x3,):
            copy.wait_send()

        def given(n):
            give_twin(n).wait_send()

        loop(tiles, given)

    def clear(c):
        acc[:, rows_at(c, 32), :] = jnp.zeros((tiles, 32, TILE), F32)

    ahead = jnp.minimum(micro, 1 + 2 * (sections - 1 - sec))

    def early(p, carry):
        normalize(p)

        @pl.when(p == 0)
        def _():
            turn_weights()

        attend(p)
        return carry

    lax.fori_loop(0, ahead, early, 0)

    def moment(p):
        sums = backward(p)

        @pl.when((sec > 0) & ((core == 0) | (p > 0)))
        def _():
            pl.semaphore_wait(go_sem, 1)

        @pl.when(sec > 0)
        def _():
            pass_down(p, *sums)

        @pl.when(p == 0)
        def _():
            loop(width // 32, clear)

        @pl.when(p < micro - 1)
        def _():
            weights(p)

        @pl.when(p == micro - 1)
        def _():
            last_weights(p)

        @pl.when((sec > 0) & ((core == 1) | (p < micro - 1)))
        def _():
            hop(p, TURN).wait_send()
            pl.semaphore_signal(go_sem, inc=1, device_id={"dp": twin}, device_id_type=MESH)

        @pl.when(p + ahead < micro)
        def _():
            normalize(p + ahead)
            attend(p + ahead)

    loop(micro, moment)
    reduce_out()

    @pl.when(sec > 0)
    def _():
        for p in range(micro - 2, micro):
            for c in range(pieces):
                if c != TURN:
                    hop(p, c).wait_send()

    @pl.when((sec > 0) & (core == 0))
    def _():
        hop(micro - 1, TURN).wait_send()


def run_pipeline(sections, lanes, counts, arrival, x, cotangent, gain, wqkv, wo):
    micro, slots, width = x.shape
    packed, head_span = wqkv.shape[1], wo.shape[1]
    tiles, cols, share = (packed + head_span) // TILE, lanes // 4, width // lanes
    vmem = pl.BlockSpec(memory_space=pltpu.VMEM)
    smem = pl.BlockSpec(memory_space=pltpu.SMEM)
    hbm = pl.BlockSpec(memory_space=pl.ANY)
    pieces = width // PIECE
    scratch = [
        pltpu.VMEM((micro, slots, width), BF16),
        pltpu.VMEM((slots, width), BF16),
        pltpu.VMEM((width, packed), BF16),
        pltpu.VMEM((packed, width), BF16),
        pltpu.VMEM((head_span, width), BF16),
        pltpu.VMEM((width, 128), F32),
        pltpu.VMEM((packed, 128), F32),
        pltpu.VMEM((micro, width, slots), BF16),
        pltpu.VMEM((micro, width, slots), BF16),
        pltpu.VMEM((micro, 8, slots), F32),
        pltpu.VMEM((micro, packed, slots), BF16),
        pltpu.VMEM((micro, HEADS, slots, slots), BF16),
        pltpu.VMEM((micro, head_span, slots), BF16),
        pltpu.VMEM((head_span, slots), BF16),
        pltpu.VMEM((head_span, slots), F32),
        pltpu.VMEM((packed, slots), BF16),
        pltpu.VMEM((tiles, width, TILE), F32),
        pltpu.VMEM((micro, width, slots), BF16),
        pltpu.VMEM((2, width, slots), BF16),
        pltpu.SemaphoreType.DMA((micro, pieces)),
        pltpu.SemaphoreType.DMA((micro, pieces)),
        pltpu.SemaphoreType.REGULAR,
        pltpu.SemaphoreType.DMA((2 + pieces + -(-head_span // PIECE),)),
        pltpu.VMEM((tiles, cols, 2, 2, share, TILE), BF16),
        pltpu.VMEM((tiles, cols, 2, share, TILE), BF16),
        pltpu.VMEM((tiles - TX, cols, share, TILE), BF16),
        pltpu.VMEM((2, TX - TX // 2, 2, share, TILE), BF16),
        pltpu.VMEM((2, TX, 2, share, TILE), BF16),
        pltpu.VMEM((2, tiles - TX - (tiles - TX) // 2, share, TILE), BF16),
        pltpu.VMEM((2, tiles - TX, share, TILE), BF16),
        pltpu.VMEM((TX, share, TILE), BF16),
        pltpu.VMEM((TX, share, TILE), BF16),
        pltpu.SemaphoreType.DMA((tiles + tiles - TX + 13,)),
        pltpu.SemaphoreType.DMA((tiles + tiles - TX + 13,)),
    ]
    return pl.pallas_call(
        functools.partial(pipeline_kernel, sections),
        out_shape=(
            jax.ShapeDtypeStruct((share, packed), F32),
            jax.ShapeDtypeStruct((share, head_span), F32),
        ),
        in_specs=[smem, smem, hbm, hbm, vmem, hbm, hbm],
        out_specs=(vmem, vmem),
        scratch_shapes=scratch,
        compiler_params=pltpu.CompilerParams(
            collective_id=0, has_side_effects=True, vmem_limit_bytes=64 * 1024 * 1024 - 65536
        ),
        name="pipeline",
    )(counts, arrival, x, cotangent, gain, wqkv, wo)


def per_device(activations, cotangent, counts, arrival, norm_gain, qkv_weight, out_weight):
    sections = lax.axis_size("section")
    qkv_share, out_share = run_pipeline(
        sections,
        lax.axis_size("dp"),
        counts[:, 0],
        arrival,
        activations[0],
        cotangent,
        norm_gain,
        qkv_weight[0],
        out_weight[0],
    )
    return (qkv_share[None], out_share[None])


def solution(mesh):
    placed = (
        P("section", None, "dp", None),
        P(None, "dp", None),
        P(None, "dp"),
        P(),
        P("section", None),
        P("section", None, None),
        P("section", None, None),
    )
    return jax.shard_map(
        per_device,
        mesh=mesh,
        in_specs=placed,
        out_specs=(P("section", "dp", None), P("section", "dp", None)),
        check_vma=False,
    )
```

```python
import functools

import jax
import jax.numpy as jnp
from jax import lax
from jax.experimental import pallas as pl
from jax.experimental.pallas import tpu as pltpu
from jax.sharding import PartitionSpec as P

HDIM = 80
HEADS = 8
EPSILON = 1e-06
MESH = pl.DeviceIdType.MESH
TILE = 256
PIECE = 256
TX = 6
TURN = 2
F32 = jnp.float32
BF16 = jnp.bfloat16


def dot_nn(a, b):
    return lax.dot_general(a, b, (((1,), (0,)), ((), ())), preferred_element_type=F32)


def dot_nt(a, b):
    return lax.dot_general(a, b, (((1,), (1,)), ((), ())), preferred_element_type=F32)


def fold(a):
    return jnp.sum(a.reshape(a.shape[0] // 8, 8, a.shape[1]), axis=0)


def loop(count, body):
    def step(i, carry):
        body(i)
        return carry

    lax.fori_loop(0, count, step, 0)


def rows_at(i, size):
    if isinstance(i, int):
        return pl.ds(i * size, size)
    return pl.ds(pl.multiple_of(i * size, size), size)


def pipeline_kernel(
    sections,
    counts_ref,
    arrival_ref,
    x_hbm,
    cot_hbm,
    gain_ref,
    wqkv_hbm,
    wo_hbm,
    out_ref,
    x_ref,
    cot_ref,
    wqkv_ref,
    wqkv_t,
    wo_t,
    gain_b,
    gain_w,
    x_t,
    hid_t,
    stats,
    pk_t,
    prob_h,
    attn_t,
    ga_t,
    ga_acc,
    gpk_t,
    acc,
    g_recv,
    g_send,
    send_sem,
    recv_sem,
    go_sem,
    load_sem,
    stage,
    got_a,
    got_y1,
    got_x1,
    got_x2,
    got_y2,
    got_y3,
    got_x3,
    send_x3,
    rs_send,
    rs_recv,
):
    micro, slots, width = x_ref.shape
    head_span = wo_hbm.shape[1]
    packed = wqkv_ref.shape[1]
    scale = HDIM**-0.5
    pieces = width // PIECE
    tiles = acc.shape[0]
    whole = packed // TILE
    edge = TILE - (packed - whole * TILE)
    sec = lax.axis_index("section")
    below = lax.rem(sec + sections - 1, sections)
    above = lax.rem(sec + 1, sections)
    lane = lax.axis_index("dp")
    core = lax.rem(lane, 2)
    twin = lane + 1 - 2 * core
    row = lax.rem(lane // 2, 2)
    col = lane // 4
    cols = stage.shape[1]
    right, left, far = (lax.rem(col + step, cols) for step in (1, cols - 1, 2))
    rest = row * 2 + core
    to_right = right * 4 + rest
    to_left = left * 4 + rest
    to_row = col * 4 + (1 - row) * 2 + core
    top = sec == sections - 1

    def load(src, dst, i):
        return pltpu.make_async_copy(src, dst, load_sem.at[i])

    def load_cot(p):
        return load(cot_hbm.at[p], cot_ref, 0)

    load_x = load(x_hbm, x_ref, 1)
    load_w = [
        load(wqkv_hbm.at[rows_at(c, PIECE)], wqkv_ref.at[rows_at(c, PIECE)], 2 + c)
        for c in range(pieces)
    ]
    wo_parts = [(at, min(PIECE, head_span - at)) for at in range(0, head_span, PIECE)]
    load_wo = [
        load(
            wo_hbm.at[:, pl.ds(at, size)],
            hid_t.at[1 + i, :, pl.ds(0, size)],
            2 + pieces + i,
        )
        for i, (at, size) in enumerate(wo_parts)
    ]
    load_x.start()
    for copy in load_w + load_wo:
        copy.start()

    @pl.when(top)
    def _():
        load_cot(0).start()

    barrier = pltpu.get_barrier_semaphore()
    for other in (below, above):
        pl.semaphore_signal(barrier, inc=1, device_id={"section": other}, device_id_type=MESH)
    for other in (twin, to_right, to_left, to_row):
        pl.semaphore_signal(barrier, inc=1, device_id={"dp": other}, device_id_type=MESH)
    pl.semaphore_wait(barrier, 6)
    gain_b[...] = jnp.broadcast_to(gain_ref[...], (128, width)).T
    load_x.wait()

    def turn_weights():
        for c in range(pieces):
            load_w[c].wait()
            wqkv_t[:, rows_at(c, PIECE)] = wqkv_ref[rows_at(c, PIECE), :].T
        for i, (at, size) in enumerate(wo_parts):
            load_wo[i].wait()
            wo_t[at : at + size, :] = hid_t[1 + i, :, 0:size].T
        gain_hi = gain_b[...].astype(BF16)
        gain_lo = (gain_b[...] - gain_hi.astype(F32)).astype(BF16)
        gains = jnp.concatenate([gain_hi, gain_lo], axis=1)

        def weigh(m):
            both = dot_nn(wqkv_t[rows_at(m, 480), :], gains) * (1.0 / width)
            gain_w[rows_at(m, 480), :] = both[:, :128] + both[:, 128:]

        loop(packed // 480, weigh)

    CH = 160
    chunks = width // CH

    def gain_rows(c, size):
        part = gain_b[rows_at(c, size), :]
        return jnp.concatenate([part] * (slots // 128), axis=1)

    def normalize(p):
        chosen = arrival_ref[p]

        def turn(c, total):
            piece = x_ref[chosen, :, rows_at(c, PIECE)].T
            x_t[p, rows_at(c, PIECE), :] = piece
            return total + fold(piece.astype(F32))

        zero = jnp.zeros((8, slots), F32)
        total = lax.fori_loop(0, pieces, turn, zero)
        mean = jnp.sum(total, axis=0, keepdims=True) * (1.0 / width)

        def add_sq(c, total):
            centered = x_t[p, rows_at(c, 320), :].astype(F32) - mean
            return total + fold(centered * centered)

        total = lax.fori_loop(0, width // 320, add_sq, zero)
        var = jnp.sum(total, axis=0, keepdims=True) * (1.0 / width)
        inv = lax.rsqrt(var + EPSILON)
        stats[p, 0:1, :] = inv
        stats[p, 1:2, :] = mean

    def attend(p):
        count = counts_ref[arrival_ref[p]]
        inv = stats[p, 0:1, :]
        mean = stats[p, 1:2, :]

        def norm(c):
            normed = (x_t[p, rows_at(c, CH), :].astype(F32) - mean) * inv
            hid_t[p, rows_at(c, CH), :] = (normed * gain_rows(c, CH)).astype(BF16)

        loop(chunks, norm)

        def pack(m):
            part = dot_nn(wqkv_t[rows_at(m, 480), :], hid_t[p])
            pk_t[p, rows_at(m, 480), :] = part.astype(BF16)

        loop(packed // 480, pack)
        keep = lax.broadcasted_iota(jnp.int32, (slots, slots), 0) < count
        for h in range(HEADS):
            q = pk_t[p, rows_at(h, HDIM), :]
            k = pk_t[p, rows_at(h + HEADS, HDIM), :]
            v = pk_t[p, rows_at(h + 2 * HEADS, HDIM), :]
            s = jnp.where(keep, dot_nn(k.T, q), -1e30)
            e = jnp.exp((s - jnp.max(s, axis=0, keepdims=True)) * scale)
            half = (e * (1.0 / jnp.sum(e, axis=0, keepdims=True))).astype(BF16)
            prob_h[p, h] = half
            attn_t[p, rows_at(h, HDIM), :] = dot_nn(v, half).astype(BF16)

    def take_cotangent(p, c):
        count = counts_ref[arrival_ref[p]]
        keep = (lax.broadcasted_iota(jnp.int32, (1, slots), 1) < count).astype(F32)
        piece = cot_ref[:, rows_at(c, PIECE)].T.astype(F32) * keep
        g_recv[p, rows_at(c, PIECE), :] = piece.astype(BF16)

    def hop(p, c):
        return pltpu.make_async_remote_copy(
            src_ref=g_send.at[lax.rem(p, 2), rows_at(c, PIECE)],
            dst_ref=g_recv.at[p, rows_at(c, PIECE)],
            send_sem=send_sem.at[p, c],
            recv_sem=recv_sem.at[p, c],
            device_id={"section": below},
            device_id_type=MESH,
        )

    def backward(p):
        @pl.when(top)
        def _():
            load_cot(p).wait()

        for c in range(pieces):

            @pl.when(top)
            def _():
                take_cotangent(p, c)

            @pl.when(jnp.logical_not(top))
            def _():
                hop(p, c).wait_recv()

            part = dot_nn(wo_t[:, rows_at(c, PIECE)], g_recv[p, rows_at(c, PIECE), :])
            if c == 0:
                ga_acc[...] = part
            elif c < pieces - 1:
                ga_acc[...] += part
            else:
                ga_t[...] = (ga_acc[...] + part).astype(BF16)

        @pl.when(top & (p < micro - 1))
        def _():
            load_cot(p + 1).start()

        first = jnp.zeros((8, slots), F32)
        second = jnp.zeros((8, slots), F32)
        for h in range(HEADS):
            q = pk_t[p, rows_at(h, HDIM), :]
            k = pk_t[p, rows_at(h + HEADS, HDIM), :]
            v = pk_t[p, rows_at(h + 2 * HEADS, HDIM), :]
            ga = ga_t[rows_at(h, HDIM), :]
            half = prob_h[p, h]
            prob = half.astype(F32)
            grad_prob = dot_nn(v.T, ga)
            inner = jnp.sum(prob * grad_prob, axis=0, keepdims=True)
            gs = (prob * (grad_prob - inner)).astype(BF16)
            grads = (dot_nn(k, gs) * scale, dot_nt(q, gs) * scale, dot_nt(ga, half))
            for i, (grad, own) in enumerate(zip(grads, (q, k, v))):
                at = rows_at(h + i * HEADS, HDIM)
                rounded = grad.astype(BF16)
                gpk_t[at, :] = rounded
                full = rounded.astype(F32)
                w = gain_w[at, :]
                first += fold(full * jnp.concatenate([w] * (slots // 128), axis=1))
                second += fold(full * own.astype(F32))
        return (
            jnp.sum(first, axis=0, keepdims=True),
            jnp.sum(second, axis=0, keepdims=True) * (1.0 / width),
        )

    def pass_down(p, first, second):
        inv = stats[p, 0:1, :]
        mean = stats[p, 1:2, :]

        @pl.when(p >= 2)
        def _():
            for c in range(pieces):
                if c != TURN:
                    hop(p - 2, c).wait_send()

        def grad_hidden(c):
            at = rows_at(c, PIECE)
            gn = dot_nn(wqkv_ref[at, :], gpk_t[...]) * gain_rows(c, PIECE)
            normed = (x_t[p, at, :].astype(F32) - mean) * inv
            grad_ln = inv * (gn - first - normed * second)
            g_send[lax.rem(p, 2), at, :] = (g_recv[p, at, :].astype(F32) + grad_ln).astype(BF16)
            hop(p, c).start()

        loop(pieces, grad_hidden)

    def tile(p, n):
        if isinstance(n, int) and n == whole:
            half = dot_nt(hid_t[p], gpk_t[n * TILE : packed, :])
            return jnp.concatenate([half, dot_nt(g_recv[p], attn_t[p, 0:edge, :])], axis=1)
        if isinstance(n, int) and n > whole:
            start = edge + (n - whole - 1) * TILE
            return dot_nt(g_recv[p], attn_t[p, start : start + TILE, :])
        return dot_nt(hid_t[p], gpk_t[rows_at(n, TILE), :])

    def weights(p):
        def qkv(n):
            acc[n] += tile(p, n)

        loop(whole, qkv)
        for n in range(whole, tiles):
            acc[n] += tile(p, n)

    def send(src, dst, i, lane_to):
        return pltpu.make_async_remote_copy(
            src_ref=src,
            dst_ref=dst,
            send_sem=rs_send.at[i],
            recv_sem=rs_recv.at[i],
            device_id={"dp": lane_to},
            device_id_type=MESH,
        )

    nx, ny = TX, tiles - TX
    hx, hy = nx // 2, ny // 2
    at_y1 = tiles
    at_x1 = at_y1 + ny
    at_x2 = at_x1 + nx
    at_x3 = at_x2 + 2 * nx
    at_y2 = at_x3 + nx
    at_y3 = at_y2 + ny
    ways = ((to_right, right), (to_left, left))

    def give_twin(n):
        return send(stage.at[n, :, :, 1 - core], got_a.at[n], n, twin)

    def copy_x1(n):
        way = n // hx
        return send(
            stage.at[n, far, :, core], got_x1.at[way, n % hx], at_x1 + n, ways[way][0]
        )

    def copy_x2(way, n):
        to, block = ways[way]
        return send(stage.at[n, block, :, core], got_x2.at[way, n], at_x2 + way * nx + n, to)

    def copy_x3(n):
        return send(send_x3.at[n], got_x3.at[n], at_x3 + n, to_row)

    def copy_y1(i):
        return send(stage.at[nx + i, :, 1 - row, core], got_y1.at[i], at_y1 + i, to_row)

    def copy_y2(i):
        way = i // hy
        return send(
            stage.at[nx + i, far, row, core], got_y2.at[way, i % hy], at_y2 + i, ways[way][0]
        )

    def copy_y3(way, i):
        to, block = ways[way]
        return send(
            stage.at[nx + i, block, row, core], got_y3.at[way, i], at_y3 + way * ny + i, to
        )

    def join(at, other):
        stage[at] = (stage[at].astype(F32) + other.astype(F32)).astype(BF16)

    def arrive(n):
        give_twin(n).wait_recv()
        for c in range(cols):
            join((n, c, slice(None), core), got_a[n, c])
        if n < nx:
            copy_x1(n).start()
            copy_x2(1 - n // hx, n).start()
        else:
            copy_y1(n - nx).start()

    def x_second(n):
        way = n // hx
        copy_x1(n).wait_recv()
        join((n, ways[way][1], slice(None), core), got_x1[way, n % hx])
        copy_x2(way, n).start()

    def across(n, r):
        total = stage[n, col, r, core].astype(F32) + got_x2[0, n, r].astype(F32)
        return total + got_x2[1, n, r].astype(F32)

    def x_third(n):
        copy_x2(0, n).wait_recv()
        copy_x2(1, n).wait_recv()
        send_x3[n] = across(n, 1 - row).astype(BF16)
        copy_x3(n).start()

    def x_last(n):
        copy_x3(n).wait_recv()
        out_ref[:, n * TILE : (n + 1) * TILE] = across(n, row) + got_x3[n].astype(F32)

    def y_first(i):
        copy_y1(i).wait_recv()
        for c in range(cols):
            join((nx + i, c, row, core), got_y1[i, c])
        copy_y2(i).start()
        copy_y3(1 - i // hy, i).start()

    def y_second(i):
        way = i // hy
        copy_y2(i).wait_recv()
        join((nx + i, ways[way][1], row, core), got_y2[way, i % hy])
        copy_y3(way, i).start()

    def y_last(i):
        copy_y3(0, i).wait_recv()
        copy_y3(1, i).wait_recv()
        n = nx + i
        total = stage[n, col, row, core].astype(F32) + got_y3[0, i].astype(F32)
        out_ref[:, n * TILE : (n + 1) * TILE] = total + got_y3[1, i].astype(F32)

    y_order = [n - nx for n in range(whole, tiles)] + list(range(whole - nx))
    x_order = [h * hx + j for j in range(hx) for h in range(2)]
    order = [nx + i for i in y_order] + x_order

    def last_weights(p):
        for n in order:
            total = (acc[n] + tile(p, n)).astype(BF16)
            stage[n] = total.reshape(stage.shape[1:])
            give_twin(n).start()

            @pl.when(core == 0)
            def _():
                arrive(n)

    def reduce_out():
        @pl.when(core == 1)
        def _():
            for n in order:
                arrive(n)

        pairs = [x_order[2 * j : 2 * j + 2] for j in range(hx)]
        for n in pairs[0]:
            x_second(n)
        y_first(y_order[0])
        for n in pairs[1]:
            x_second(n)
        y_first(y_order[1])
        for n in pairs[2]:
            x_second(n)
        y_second(y_order[0])
        y_first(y_order[2])
        y_second(y_order[1])
        for n in pairs[0]:
            x_third(n)
        y_first(y_order[3])
        y_second(y_order[2])
        for n in pairs[1]:
            x_third(n)
        y_second(y_order[3])
        for n in pairs[2]:
            x_third(n)
        for i in y_order:
            y_last(i)
        for n in x_order:
            x_last(n)
        for n in range(tiles):
            give_twin(n).wait_send()
        for n in range(nx):
            for copy in (copy_x1(n), copy_x2(0, n), copy_x2(1, n), copy_x3(n)):
                copy.wait_send()
        for i in range(ny):
            for copy in (copy_y1(i), copy_y2(i), copy_y3(0, i), copy_y3(1, i)):
                copy.wait_send()

    def clear(c):
        acc[:, rows_at(c, 32), :] = jnp.zeros((tiles, 32, TILE), F32)

    ahead = jnp.minimum(micro, 1 + 2 * (sections - 1 - sec))

    def early(p, carry):
        normalize(p)

        @pl.when(p == 0)
        def _():
            turn_weights()

        attend(p)
        return carry

    lax.fori_loop(0, ahead, early, 0)

    def moment(p):
        sums = backward(p)

        @pl.when((sec > 0) & ((core == 0) | (p > 0)))
        def _():
            pl.semaphore_wait(go_sem, 1)

        @pl.when(sec > 0)
        def _():
            pass_down(p, *sums)

        @pl.when(p == 0)
        def _():
            loop(width // 32, clear)

        @pl.when(p < micro - 1)
        def _():
            weights(p)

        @pl.when(p == micro - 1)
        def _():
            last_weights(p)

        @pl.when((sec > 0) & ((core == 1) | (p < micro - 1)))
        def _():
            hop(p, TURN).wait_send()
            pl.semaphore_signal(go_sem, inc=1, device_id={"dp": twin}, device_id_type=MESH)

        @pl.when(p + ahead < micro)
        def _():
            normalize(p + ahead)
            attend(p + ahead)

    loop(micro, moment)
    reduce_out()

    @pl.when(sec > 0)
    def _():
        for p in range(micro - 2, micro):
            for c in range(pieces):
                if c != TURN:
                    hop(p, c).wait_send()

    @pl.when((sec > 0) & (core == 0))
    def _():
        hop(micro - 1, TURN).wait_send()


def run_pipeline(sections, lanes, counts, arrival, x, cotangent, gain, wqkv, wo):
    micro, slots, width = x.shape
    packed, head_span = wqkv.shape[1], wo.shape[1]
    tiles, cols, share = (packed + head_span) // TILE, lanes // 4, width // lanes
    vmem = pl.BlockSpec(memory_space=pltpu.VMEM)
    smem = pl.BlockSpec(memory_space=pltpu.SMEM)
    hbm = pl.BlockSpec(memory_space=pl.ANY)
    pieces = width // PIECE
    scratch = [
        pltpu.VMEM((micro, slots, width), BF16),
        pltpu.VMEM((slots, width), BF16),
        pltpu.VMEM((width, packed), BF16),
        pltpu.VMEM((packed, width), BF16),
        pltpu.VMEM((head_span, width), BF16),
        pltpu.VMEM((width, 128), F32),
        pltpu.VMEM((packed, 128), F32),
        pltpu.VMEM((micro, width, slots), BF16),
        pltpu.VMEM((micro, width, slots), BF16),
        pltpu.VMEM((micro, 8, slots), F32),
        pltpu.VMEM((micro, packed, slots), BF16),
        pltpu.VMEM((micro, HEADS, slots, slots), BF16),
        pltpu.VMEM((micro, head_span, slots), BF16),
        pltpu.VMEM((head_span, slots), BF16),
        pltpu.VMEM((head_span, slots), F32),
        pltpu.VMEM((packed, slots), BF16),
        pltpu.VMEM((tiles, width, TILE), F32),
        pltpu.VMEM((micro, width, slots), BF16),
        pltpu.VMEM((2, width, slots), BF16),
        pltpu.SemaphoreType.DMA((micro, pieces)),
        pltpu.SemaphoreType.DMA((micro, pieces)),
        pltpu.SemaphoreType.REGULAR,
        pltpu.SemaphoreType.DMA((2 + pieces + -(-head_span // PIECE),)),
        pltpu.VMEM((tiles, cols, 2, 2, share, TILE), BF16),
        pltpu.VMEM((tiles, cols, 2, share, TILE), BF16),
        pltpu.VMEM((tiles - TX, cols, share, TILE), BF16),
        pltpu.VMEM((2, TX - TX // 2, 2, share, TILE), BF16),
        pltpu.VMEM((2, TX, 2, share, TILE), BF16),
        pltpu.VMEM((2, tiles - TX - (tiles - TX) // 2, share, TILE), BF16),
        pltpu.VMEM((2, tiles - TX, share, TILE), BF16),
        pltpu.VMEM((TX, share, TILE), BF16),
        pltpu.VMEM((TX, share, TILE), BF16),
        pltpu.SemaphoreType.DMA((tiles + 4 * TX + 4 * (tiles - TX),)),
        pltpu.SemaphoreType.DMA((tiles + 4 * TX + 4 * (tiles - TX),)),
    ]
    return pl.pallas_call(
        functools.partial(pipeline_kernel, sections),
        out_shape=jax.ShapeDtypeStruct((share, packed + head_span), F32),
        in_specs=[smem, smem, hbm, hbm, vmem, hbm, hbm],
        out_specs=vmem,
        scratch_shapes=scratch,
        compiler_params=pltpu.CompilerParams(
            collective_id=0, has_side_effects=True, vmem_limit_bytes=64 * 1024 * 1024 - 65536
        ),
        name="pipeline",
    )(counts, arrival, x, cotangent, gain, wqkv, wo)


def split_kernel(both_ref, qkv_ref, out_ref):
    packed = qkv_ref.shape[1]
    qkv_ref[...] = both_ref[:, :packed]
    out_ref[...] = both_ref[:, packed:]


def per_device(activations, cotangent, counts, arrival, norm_gain, qkv_weight, out_weight):
    sections = lax.axis_size("section")
    packed = qkv_weight.shape[2]
    both = run_pipeline(
        sections,
        lax.axis_size("dp"),
        counts[:, 0],
        arrival,
        activations[0],
        cotangent,
        norm_gain,
        qkv_weight[0],
        out_weight[0],
    )
    share, width = both.shape
    vmem = pl.BlockSpec(memory_space=pltpu.VMEM)
    qkv_share, out_share = pl.pallas_call(
        split_kernel,
        out_shape=(
            jax.ShapeDtypeStruct((share, packed), F32),
            jax.ShapeDtypeStruct((share, width - packed), F32),
        ),
        in_specs=[vmem],
        out_specs=(vmem, vmem),
        name="split",
    )(both)
    return (qkv_share[None], out_share[None])


def solution(mesh):
    placed = (
        P("section", None, "dp", None),
        P(None, "dp", None),
        P(None, "dp"),
        P(),
        P("section", None),
        P("section", None, None),
        P("section", None, None),
    )
    return jax.shard_map(
        per_device,
        mesh=mesh,
        in_specs=placed,
        out_specs=(P("section", "dp", None), P("section", "dp", None)),
        check_vma=False,
    )
```

```python
import functools

import jax
import jax.numpy as jnp
from jax import lax
from jax.experimental import pallas as pl
from jax.experimental.pallas import tpu as pltpu
from jax.sharding import PartitionSpec as P

HDIM = 80
HEADS = 8
EPSILON = 1e-06
MESH = pl.DeviceIdType.MESH
TILE = 256
PIECE = 256
TX = 6
TURN = 3
F32 = jnp.float32
BF16 = jnp.bfloat16


def dot_nn(a, b):
    return lax.dot_general(a, b, (((1,), (0,)), ((), ())), preferred_element_type=F32)


def dot_nt(a, b):
    return lax.dot_general(a, b, (((1,), (1,)), ((), ())), preferred_element_type=F32)


def fold(a):
    return jnp.sum(a.reshape(a.shape[0] // 8, 8, a.shape[1]), axis=0)


def loop(count, body):
    def step(i, carry):
        body(i)
        return carry

    lax.fori_loop(0, count, step, 0)


def rows_at(i, size):
    if isinstance(i, int):
        return pl.ds(i * size, size)
    return pl.ds(pl.multiple_of(i * size, size), size)


def pipeline_kernel(
    sections,
    counts_ref,
    arrival_ref,
    x_hbm,
    cot_hbm,
    gain_ref,
    wqkv_hbm,
    wo_hbm,
    out_ref,
    x_ref,
    cot_ref,
    wqkv_ref,
    wqkv_t,
    wo_t,
    gain_b,
    gain_w,
    x_t,
    hid_t,
    stats,
    pk_t,
    prob_h,
    attn_t,
    ga_t,
    ga_acc,
    gpk_t,
    acc,
    g_recv,
    g_send,
    send_sem,
    recv_sem,
    go_sem,
    load_sem,
    stage,
    got_a,
    got_y1,
    got_x1,
    got_x2,
    got_y2,
    got_y3,
    got_x3,
    send_x3,
    rs_send,
    rs_recv,
):
    micro, slots, width = x_ref.shape
    head_span = wo_hbm.shape[1]
    packed = wqkv_ref.shape[1]
    scale = HDIM**-0.5
    pieces = width // PIECE
    tiles = acc.shape[0]
    whole = packed // TILE
    edge = TILE - (packed - whole * TILE)
    sec = lax.axis_index("section")
    below = lax.rem(sec + sections - 1, sections)
    above = lax.rem(sec + 1, sections)
    lane = lax.axis_index("dp")
    core = lax.rem(lane, 2)
    twin = lane + 1 - 2 * core
    row = lax.rem(lane // 2, 2)
    col = lane // 4
    cols = stage.shape[1]
    right, left, far = (lax.rem(col + step, cols) for step in (1, cols - 1, 2))
    rest = row * 2 + core
    to_right = right * 4 + rest
    to_left = left * 4 + rest
    to_row = col * 4 + (1 - row) * 2 + core
    top = sec == sections - 1

    def load(src, dst, i):
        return pltpu.make_async_copy(src, dst, load_sem.at[i])

    def load_cot(p):
        return load(cot_hbm.at[p], cot_ref, 0)

    load_x = load(x_hbm, x_ref, 1)
    load_w = [
        load(wqkv_hbm.at[rows_at(c, PIECE)], wqkv_ref.at[rows_at(c, PIECE)], 2 + c)
        for c in range(pieces)
    ]
    wo_parts = [(at, min(PIECE, head_span - at)) for at in range(0, head_span, PIECE)]
    load_wo = [
        load(
            wo_hbm.at[:, pl.ds(at, size)],
            hid_t.at[1 + i, :, pl.ds(0, size)],
            2 + pieces + i,
        )
        for i, (at, size) in enumerate(wo_parts)
    ]
    load_x.start()
    for copy in load_w + load_wo:
        copy.start()

    @pl.when(top)
    def _():
        load_cot(0).start()

    barrier = pltpu.get_barrier_semaphore()
    for other in (below, above):
        pl.semaphore_signal(barrier, inc=1, device_id={"section": other}, device_id_type=MESH)
    for other in (twin, to_right, to_left, to_row):
        pl.semaphore_signal(barrier, inc=1, device_id={"dp": other}, device_id_type=MESH)
    gain_b[...] = jnp.broadcast_to(gain_ref[...], (128, width)).T
    load_x.wait()

    def turn_weights():
        for c in range(pieces):
            load_w[c].wait()
            wqkv_t[:, rows_at(c, PIECE)] = wqkv_ref[rows_at(c, PIECE), :].T
        for i, (at, size) in enumerate(wo_parts):
            load_wo[i].wait()
            wo_t[at : at + size, :] = hid_t[1 + i, :, 0:size].T
        gains = jnp.broadcast_to(gain_ref[...], (16, width))
        high = gains.astype(BF16).astype(F32)
        at_row = lax.broadcasted_iota(jnp.int32, (16, width), 0)
        gains = jnp.where(at_row == 0, high, jnp.where(at_row == 1, gains - high, 0.0))
        sums = dot_nn(gains.astype(BF16), wqkv_ref[...])
        sums = jnp.sum(sums, axis=0, keepdims=True) * (1.0 / width)
        gain_w[...] = jnp.broadcast_to(sums, (128, packed)).T

    CH = 160
    chunks = width // CH

    def gain_rows(c, size):
        part = gain_b[rows_at(c, size), :]
        return jnp.concatenate([part] * (slots // 128), axis=1)

    def normalize(p):
        chosen = arrival_ref[p]

        def turn(c, total):
            piece = x_ref[chosen, :, rows_at(c, PIECE)].T
            x_t[p, rows_at(c, PIECE), :] = piece
            return total + fold(piece.astype(F32))

        zero = jnp.zeros((8, slots), F32)
        total = lax.fori_loop(0, pieces, turn, zero)
        mean = jnp.sum(total, axis=0, keepdims=True) * (1.0 / width)

        def add_sq(c, total):
            centered = x_t[p, rows_at(c, 320), :].astype(F32) - mean
            return total + fold(centered * centered)

        total = lax.fori_loop(0, width // 320, add_sq, zero)
        var = jnp.sum(total, axis=0, keepdims=True) * (1.0 / width)
        inv = lax.rsqrt(var + EPSILON)
        stats[p, 0:1, :] = inv
        stats[p, 1:2, :] = mean

    def attend(p):
        count = counts_ref[arrival_ref[p]]
        inv = stats[p, 0:1, :]
        mean = stats[p, 1:2, :]

        def norm(c):
            normed = (x_t[p, rows_at(c, CH), :].astype(F32) - mean) * inv
            hid_t[p, rows_at(c, CH), :] = (normed * gain_rows(c, CH)).astype(BF16)

        loop(chunks, norm)

        def pack(m):
            part = dot_nn(wqkv_t[rows_at(m, 480), :], hid_t[p])
            pk_t[p, rows_at(m, 480), :] = part.astype(BF16)

        loop(packed // 480, pack)
        keep = lax.broadcasted_iota(jnp.int32, (slots, slots), 0) < count
        for h in range(HEADS):
            q = pk_t[p, rows_at(h, HDIM), :]
            k = pk_t[p, rows_at(h + HEADS, HDIM), :]
            v = pk_t[p, rows_at(h + 2 * HEADS, HDIM), :]
            s = jnp.where(keep, dot_nn(k.T, q), -1e30)
            e = jnp.exp((s - jnp.max(s, axis=0, keepdims=True)) * scale)
            half = (e * (1.0 / jnp.sum(e, axis=0, keepdims=True))).astype(BF16)
            prob_h[p, h] = half
            attn_t[p, rows_at(h, HDIM), :] = dot_nn(v, half).astype(BF16)

    def take_cotangent(p, c):
        count = counts_ref[arrival_ref[p]]
        keep = (lax.broadcasted_iota(jnp.int32, (1, slots), 1) < count).astype(F32)
        piece = cot_ref[:, rows_at(c, PIECE)].T.astype(F32) * keep
        g_recv[p, rows_at(c, PIECE), :] = piece.astype(BF16)

    def hop(p, c):
        return pltpu.make_async_remote_copy(
            src_ref=g_send.at[lax.rem(p, 2), rows_at(c, PIECE)],
            dst_ref=g_recv.at[p, rows_at(c, PIECE)],
            send_sem=send_sem.at[p, c],
            recv_sem=recv_sem.at[p, c],
            device_id={"section": below},
            device_id_type=MESH,
        )

    def backward(p):
        @pl.when(top)
        def _():
            load_cot(p).wait()

        for c in range(pieces):

            @pl.when(top)
            def _():
                take_cotangent(p, c)

            @pl.when(jnp.logical_not(top))
            def _():
                hop(p, c).wait_recv()

            part = dot_nn(wo_t[:, rows_at(c, PIECE)], g_recv[p, rows_at(c, PIECE), :])
            if c == 0:
                ga_acc[...] = part
            elif c < pieces - 1:
                ga_acc[...] += part
            else:
                ga_t[...] = (ga_acc[...] + part).astype(BF16)

        @pl.when(top & (p < micro - 1))
        def _():
            load_cot(p + 1).start()

        first = jnp.zeros((8, slots), F32)
        second = jnp.zeros((8, slots), F32)
        for h in range(HEADS):
            q = pk_t[p, rows_at(h, HDIM), :]
            k = pk_t[p, rows_at(h + HEADS, HDIM), :]
            v = pk_t[p, rows_at(h + 2 * HEADS, HDIM), :]
            ga = ga_t[rows_at(h, HDIM), :]
            half = prob_h[p, h]
            prob = half.astype(F32)
            grad_prob = dot_nn(v.T, ga)
            inner = jnp.sum(prob * grad_prob, axis=0, keepdims=True)
            gs = (prob * (grad_prob - inner)).astype(BF16)
            grads = (dot_nn(k, gs) * scale, dot_nt(q, gs) * scale, dot_nt(ga, half))
            for i, (grad, own) in enumerate(zip(grads, (q, k, v))):
                at = rows_at(h + i * HEADS, HDIM)
                rounded = grad.astype(BF16)
                gpk_t[at, :] = rounded
                full = rounded.astype(F32)
                w = gain_w[at, :]
                first += fold(full * jnp.concatenate([w] * (slots // 128), axis=1))
                second += fold(full * own.astype(F32))
        return (
            jnp.sum(first, axis=0, keepdims=True),
            jnp.sum(second, axis=0, keepdims=True) * (1.0 / width),
        )

    def pass_down(p, first, second):
        inv = stats[p, 0:1, :]
        mean = stats[p, 1:2, :]

        @pl.when(p >= 2)
        def _():
            for c in range(pieces):
                if c != TURN:
                    hop(p - 2, c).wait_send()

        def grad_hidden(c):
            at = rows_at(c, PIECE)
            gn = dot_nn(wqkv_ref[at, :], gpk_t[...]) * gain_rows(c, PIECE)
            normed = (x_t[p, at, :].astype(F32) - mean) * inv
            grad_ln = inv * (gn - first - normed * second)
            g_send[lax.rem(p, 2), at, :] = (g_recv[p, at, :].astype(F32) + grad_ln).astype(BF16)
            hop(p, c).start()

        loop(pieces, grad_hidden)

    def tile(p, n):
        if isinstance(n, int) and n == whole:
            half = dot_nt(hid_t[p], gpk_t[n * TILE : packed, :])
            return jnp.concatenate([half, dot_nt(g_recv[p], attn_t[p, 0:edge, :])], axis=1)
        if isinstance(n, int) and n > whole:
            start = edge + (n - whole - 1) * TILE
            return dot_nt(g_recv[p], attn_t[p, start : start + TILE, :])
        return dot_nt(hid_t[p], gpk_t[rows_at(n, TILE), :])

    def weights(p):
        def qkv(n):
            acc[n] += tile(p, n)

        loop(whole, qkv)
        for n in range(whole, tiles):
            acc[n] += tile(p, n)

    def send(src, dst, i, lane_to):
        return pltpu.make_async_remote_copy(
            src_ref=src,
            dst_ref=dst,
            send_sem=rs_send.at[i],
            recv_sem=rs_recv.at[i],
            device_id={"dp": lane_to},
            device_id_type=MESH,
        )

    nx, ny = TX, tiles - TX
    hx, hy = nx // 2, ny // 2
    at_y1 = tiles
    at_x1 = at_y1 + ny
    at_x2 = at_x1 + nx
    at_x3 = at_x2 + 2 * nx
    at_y2 = at_x3 + nx
    at_y3 = at_y2 + ny
    ways = ((to_right, right), (to_left, left))

    def give_twin(n):
        return send(stage.at[n, :, :, 1 - core], got_a.at[n], n, twin)

    def copy_x1(n):
        way = n // hx
        return send(
            stage.at[n, far, :, core], got_x1.at[way, n % hx], at_x1 + n, ways[way][0]
        )

    def copy_x2(way, n):
        to, block = ways[way]
        return send(stage.at[n, block, :, core], got_x2.at[way, n], at_x2 + way * nx + n, to)

    def copy_x3(n):
        return send(send_x3.at[n], got_x3.at[n], at_x3 + n, to_row)

    def copy_y1(i):
        return send(stage.at[nx + i, :, 1 - row, core], got_y1.at[i], at_y1 + i, to_row)

    def copy_y2(i):
        way = i // hy
        return send(
            stage.at[nx + i, far, row, core], got_y2.at[way, i % hy], at_y2 + i, ways[way][0]
        )

    def copy_y3(way, i):
        to, block = ways[way]
        return send(
            stage.at[nx + i, block, row, core], got_y3.at[way, i], at_y3 + way * ny + i, to
        )

    def join(at, other):
        stage[at] = (stage[at].astype(F32) + other.astype(F32)).astype(BF16)

    def arrive(n):
        give_twin(n).wait_recv()
        for c in range(cols):
            join((n, c, slice(None), core), got_a[n, c])
        if n < nx:
            copy_x1(n).start()
        else:
            copy_y1(n - nx).start()

    def x_second(n):
        way = n // hx
        copy_x1(n).wait_recv()
        copy_x2(1 - way, n).start()
        join((n, ways[way][1], slice(None), core), got_x1[way, n % hx])
        copy_x2(way, n).start()

    def across(n, r):
        total = stage[n, col, r, core].astype(F32) + got_x2[0, n, r].astype(F32)
        return total + got_x2[1, n, r].astype(F32)

    def x_third(n):
        copy_x2(0, n).wait_recv()
        copy_x2(1, n).wait_recv()
        send_x3[n] = across(n, 1 - row).astype(BF16)
        copy_x3(n).start()

    def x_last(n):
        copy_x3(n).wait_recv()
        out_ref[:, n * TILE : (n + 1) * TILE] = across(n, row) + got_x3[n].astype(F32)

    def y_first(i):
        copy_y1(i).wait_recv()
        for c in range(cols):
            join((nx + i, c, row, core), got_y1[i, c])
        copy_y2(i).start()
        copy_y3(1 - i // hy, i).start()

    def y_second(i):
        way = i // hy
        copy_y2(i).wait_recv()
        join((nx + i, ways[way][1], row, core), got_y2[way, i % hy])
        copy_y3(way, i).start()

    def y_last(i):
        copy_y3(0, i).wait_recv()
        copy_y3(1, i).wait_recv()
        n = nx + i
        total = stage[n, col, row, core].astype(F32) + got_y3[0, i].astype(F32)
        out_ref[:, n * TILE : (n + 1) * TILE] = total + got_y3[1, i].astype(F32)

    y_order = [n - nx for n in range(whole, tiles)] + list(range(whole - nx))
    x_order = [h * hx + j for j in range(hx) for h in range(2)]
    order = [nx + i for i in y_order] + x_order

    def last_weights(p):
        for n in order:
            total = (acc[n] + tile(p, n)).astype(BF16)
            stage[n] = total.reshape(stage.shape[1:])
            give_twin(n).start()

            @pl.when(core == 0)
            def _():
                arrive(n)

    def reduce_out():
        @pl.when(core == 1)
        def _():
            for n in order:
                arrive(n)

        pairs = [x_order[2 * j : 2 * j + 2] for j in range(hx)]
        for n in pairs[0]:
            x_second(n)
        y_first(y_order[0])
        for n in pairs[1]:
            x_second(n)
        y_first(y_order[1])
        for n in pairs[2]:
            x_second(n)
        y_second(y_order[0])
        y_first(y_order[2])
        y_second(y_order[1])
        for n in pairs[0]:
            x_third(n)
        y_first(y_order[3])
        y_second(y_order[2])
        for n in pairs[1]:
            x_third(n)
        y_second(y_order[3])
        for n in pairs[2]:
            x_third(n)
        for i in y_order:
            y_last(i)
        for n in x_order:
            x_last(n)
        for n in range(tiles):
            give_twin(n).wait_send()
        for n in range(nx):
            for copy in (copy_x1(n), copy_x2(0, n), copy_x2(1, n), copy_x3(n)):
                copy.wait_send()
        for i in range(ny):
            for copy in (copy_y1(i), copy_y2(i), copy_y3(0, i), copy_y3(1, i)):
                copy.wait_send()

    def clear(c):
        acc[:, rows_at(c, 32), :] = jnp.zeros((tiles, 32, TILE), F32)

    ahead = jnp.minimum(micro, 1 + 2 * (sections - 1 - sec))

    def early(p, carry):
        normalize(p)

        @pl.when(p == 0)
        def _():
            turn_weights()

        attend(p)
        return carry

    lax.fori_loop(0, ahead, early, 0)
    pl.semaphore_wait(barrier, 6)

    def moment(p):
        sums = backward(p)

        @pl.when((sec > 0) & ((core == 0) | (p > 0)))
        def _():
            pl.semaphore_wait(go_sem, 1)

        @pl.when(sec > 0)
        def _():
            pass_down(p, *sums)

        @pl.when(p == 0)
        def _():
            loop(width // 32, clear)

        @pl.when(p < micro - 1)
        def _():
            weights(p)

        @pl.when(p == micro - 1)
        def _():
            last_weights(p)

        @pl.when((sec > 0) & ((core == 1) | (p < micro - 1)))
        def _():
            hop(p, TURN).wait_send()
            pl.semaphore_signal(go_sem, inc=1, device_id={"dp": twin}, device_id_type=MESH)

        @pl.when(p + ahead < micro)
        def _():
            normalize(p + ahead)
            attend(p + ahead)

    loop(micro, moment)
    reduce_out()

    @pl.when(sec > 0)
    def _():
        for p in range(micro - 2, micro):
            for c in range(pieces):
                if c != TURN:
                    hop(p, c).wait_send()

    @pl.when((sec > 0) & (core == 0))
    def _():
        hop(micro - 1, TURN).wait_send()


def run_pipeline(sections, lanes, counts, arrival, x, cotangent, gain, wqkv, wo):
    micro, slots, width = x.shape
    packed, head_span = wqkv.shape[1], wo.shape[1]
    tiles, cols, share = (packed + head_span) // TILE, lanes // 4, width // lanes
    vmem = pl.BlockSpec(memory_space=pltpu.VMEM)
    smem = pl.BlockSpec(memory_space=pltpu.SMEM)
    hbm = pl.BlockSpec(memory_space=pl.ANY)
    pieces = width // PIECE
    scratch = [
        pltpu.VMEM((micro, slots, width), BF16),
        pltpu.VMEM((slots, width), BF16),
        pltpu.VMEM((width, packed), BF16),
        pltpu.VMEM((packed, width), BF16),
        pltpu.VMEM((head_span, width), BF16),
        pltpu.VMEM((width, 128), F32),
        pltpu.VMEM((packed, 128), F32),
        pltpu.VMEM((micro, width, slots), BF16),
        pltpu.VMEM((micro, width, slots), BF16),
        pltpu.VMEM((micro, 8, slots), F32),
        pltpu.VMEM((micro, packed, slots), BF16),
        pltpu.VMEM((micro, HEADS, slots, slots), BF16),
        pltpu.VMEM((micro, head_span, slots), BF16),
        pltpu.VMEM((head_span, slots), BF16),
        pltpu.VMEM((head_span, slots), F32),
        pltpu.VMEM((packed, slots), BF16),
        pltpu.VMEM((tiles, width, TILE), F32),
        pltpu.VMEM((micro, width, slots), BF16),
        pltpu.VMEM((2, width, slots), BF16),
        pltpu.SemaphoreType.DMA((micro, pieces)),
        pltpu.SemaphoreType.DMA((micro, pieces)),
        pltpu.SemaphoreType.REGULAR,
        pltpu.SemaphoreType.DMA((2 + pieces + -(-head_span // PIECE),)),
        pltpu.VMEM((tiles, cols, 2, 2, share, TILE), BF16),
        pltpu.VMEM((tiles, cols, 2, share, TILE), BF16),
        pltpu.VMEM((tiles - TX, cols, share, TILE), BF16),
        pltpu.VMEM((2, TX - TX // 2, 2, share, TILE), BF16),
        pltpu.VMEM((2, TX, 2, share, TILE), BF16),
        pltpu.VMEM((2, tiles - TX - (tiles - TX) // 2, share, TILE), BF16),
        pltpu.VMEM((2, tiles - TX, share, TILE), BF16),
        pltpu.VMEM((TX, share, TILE), BF16),
        pltpu.VMEM((TX, share, TILE), BF16),
        pltpu.SemaphoreType.DMA((tiles + 4 * TX + 4 * (tiles - TX),)),
        pltpu.SemaphoreType.DMA((tiles + 4 * TX + 4 * (tiles - TX),)),
    ]
    return pl.pallas_call(
        functools.partial(pipeline_kernel, sections),
        out_shape=jax.ShapeDtypeStruct((share, packed + head_span), F32),
        in_specs=[smem, smem, hbm, hbm, vmem, hbm, hbm],
        out_specs=vmem,
        scratch_shapes=scratch,
        compiler_params=pltpu.CompilerParams(
            collective_id=0, has_side_effects=True, vmem_limit_bytes=64 * 1024 * 1024 - 65536
        ),
        name="pipeline",
    )(counts, arrival, x, cotangent, gain, wqkv, wo)


def split_kernel(both_ref, qkv_ref, out_ref):
    packed = qkv_ref.shape[1]
    qkv_ref[...] = both_ref[:, :packed]
    out_ref[...] = both_ref[:, packed:]


def per_device(activations, cotangent, counts, arrival, norm_gain, qkv_weight, out_weight):
    sections = lax.axis_size("section")
    packed = qkv_weight.shape[2]
    both = run_pipeline(
        sections,
        lax.axis_size("dp"),
        counts[:, 0],
        arrival,
        activations[0],
        cotangent,
        norm_gain,
        qkv_weight[0],
        out_weight[0],
    )
    share, width = both.shape
    vmem = pl.BlockSpec(memory_space=pltpu.VMEM)
    qkv_share, out_share = pl.pallas_call(
        split_kernel,
        out_shape=(
            jax.ShapeDtypeStruct((share, packed), F32),
            jax.ShapeDtypeStruct((share, width - packed), F32),
        ),
        in_specs=[vmem],
        out_specs=(vmem, vmem),
        name="split",
    )(both)
    return (qkv_share[None], out_share[None])


def solution(mesh):
    placed = (
        P("section", None, "dp", None),
        P(None, "dp", None),
        P(None, "dp"),
        P(),
        P("section", None),
        P("section", None, None),
        P("section", None, None),
    )
    return jax.shard_map(
        per_device,
        mesh=mesh,
        in_specs=placed,
        out_specs=(P("section", "dp", None), P("section", "dp", None)),
        check_vma=False,
    )
```

```python
import functools

import jax
import jax.numpy as jnp
from jax import lax
from jax.experimental import pallas as pl
from jax.experimental.pallas import tpu as pltpu
from jax.sharding import PartitionSpec as P

HDIM = 80
HEADS = 8
EPSILON = 1e-06
MESH = pl.DeviceIdType.MESH
TILE = 256
PIECE = 256
TX = 6
TURN = 2
F32 = jnp.float32
BF16 = jnp.bfloat16


def dot_nn(a, b):
    return lax.dot_general(a, b, (((1,), (0,)), ((), ())), preferred_element_type=F32)


def dot_nt(a, b):
    return lax.dot_general(a, b, (((1,), (1,)), ((), ())), preferred_element_type=F32)


def fold(a):
    return jnp.sum(a.reshape(a.shape[0] // 8, 8, a.shape[1]), axis=0)


def loop(count, body):
    def step(i, carry):
        body(i)
        return carry

    lax.fori_loop(0, count, step, 0)


def rows_at(i, size):
    if isinstance(i, int):
        return pl.ds(i * size, size)
    return pl.ds(pl.multiple_of(i * size, size), size)


def pipeline_kernel(
    sections,
    counts_ref,
    arrival_ref,
    x_hbm,
    cot_hbm,
    gain_ref,
    wqkv_hbm,
    wo_hbm,
    out_ref,
    x_ref,
    cot_ref,
    wqkv_ref,
    wqkv_t,
    wo_t,
    gain_b,
    gain_w,
    x_t,
    hid_t,
    stats,
    pk_t,
    prob_h,
    attn_t,
    ga_t,
    ga_acc,
    gpk_t,
    acc,
    g_recv,
    g_send,
    send_sem,
    recv_sem,
    go_sem,
    load_sem,
    stage,
    got_a,
    got_y1,
    got_x1,
    got_x2,
    got_y2,
    got_y3,
    got_x3,
    send_x3,
    rs_send,
    rs_recv,
):
    micro, slots, width = x_ref.shape
    head_span = wo_hbm.shape[1]
    packed = wqkv_ref.shape[1]
    scale = HDIM**-0.5
    pieces = width // PIECE
    tiles = acc.shape[0]
    whole = packed // TILE
    edge = TILE - (packed - whole * TILE)
    sec = lax.axis_index("section")
    below = lax.rem(sec + sections - 1, sections)
    above = lax.rem(sec + 1, sections)
    lane = lax.axis_index("dp")
    core = lax.rem(lane, 2)
    twin = lane + 1 - 2 * core
    row = lax.rem(lane // 2, 2)
    col = lane // 4
    cols = stage.shape[1]
    right, left, far = (lax.rem(col + step, cols) for step in (1, cols - 1, 2))
    rest = row * 2 + core
    to_right = right * 4 + rest
    to_left = left * 4 + rest
    to_row = col * 4 + (1 - row) * 2 + core
    top = sec == sections - 1

    def load(src, dst, i):
        return pltpu.make_async_copy(src, dst, load_sem.at[i])

    def load_cot(p):
        return load(cot_hbm.at[p], cot_ref, 0)

    load_x = load(x_hbm, x_ref, 1)
    load_w = [
        load(wqkv_hbm.at[rows_at(c, PIECE)], wqkv_ref.at[rows_at(c, PIECE)], 2 + c)
        for c in range(pieces)
    ]
    wo_parts = [(at, min(PIECE, head_span - at)) for at in range(0, head_span, PIECE)]
    load_wo = [
        load(
            wo_hbm.at[:, pl.ds(at, size)],
            hid_t.at[1 + i, :, pl.ds(0, size)],
            2 + pieces + i,
        )
        for i, (at, size) in enumerate(wo_parts)
    ]
    load_x.start()
    for copy in load_w + load_wo:
        copy.start()

    @pl.when(top)
    def _():
        load_cot(0).start()

    barrier = pltpu.get_barrier_semaphore()
    for other in (below, above):
        pl.semaphore_signal(barrier, inc=1, device_id={"section": other}, device_id_type=MESH)
    for other in (twin, to_right, to_left, to_row):
        pl.semaphore_signal(barrier, inc=1, device_id={"dp": other}, device_id_type=MESH)
    gain_b[...] = jnp.broadcast_to(gain_ref[...], (128, width)).T
    load_x.wait()

    def turn_weights():
        for c in range(pieces):
            load_w[c].wait()
            wqkv_t[:, rows_at(c, PIECE)] = wqkv_ref[rows_at(c, PIECE), :].T
        for i, (at, size) in enumerate(wo_parts):
            load_wo[i].wait()
            wo_t[at : at + size, :] = hid_t[1 + i, :, 0:size].T
        gains = jnp.broadcast_to(gain_ref[...], (16, width))
        high = gains.astype(BF16).astype(F32)
        at_row = lax.broadcasted_iota(jnp.int32, (16, width), 0)
        gains = jnp.where(at_row == 0, high, jnp.where(at_row == 1, gains - high, 0.0))
        sums = dot_nn(gains.astype(BF16), wqkv_ref[...])
        sums = jnp.sum(sums, axis=0, keepdims=True) * (1.0 / width)
        gain_w[...] = jnp.broadcast_to(sums, (128, packed)).T

    CH = 160
    chunks = width // CH

    def gain_rows(c, size):
        part = gain_b[rows_at(c, size), :]
        return jnp.concatenate([part] * (slots // 128), axis=1)

    def normalize(p):
        chosen = arrival_ref[p]

        def turn(c, total):
            piece = x_ref[chosen, :, rows_at(c, PIECE)].T
            x_t[p, rows_at(c, PIECE), :] = piece
            return total + fold(piece.astype(F32))

        zero = jnp.zeros((8, slots), F32)
        total = lax.fori_loop(0, pieces, turn, zero)
        mean = jnp.sum(total, axis=0, keepdims=True) * (1.0 / width)

        def add_sq(c, total):
            centered = x_t[p, rows_at(c, 320), :].astype(F32) - mean
            return total + fold(centered * centered)

        total = lax.fori_loop(0, width // 320, add_sq, zero)
        var = jnp.sum(total, axis=0, keepdims=True) * (1.0 / width)
        inv = lax.rsqrt(var + EPSILON)
        stats[p, 0:1, :] = inv
        stats[p, 1:2, :] = mean

    def attend(p):
        count = counts_ref[arrival_ref[p]]
        inv = stats[p, 0:1, :]
        mean = stats[p, 1:2, :]

        def norm(c):
            normed = (x_t[p, rows_at(c, CH), :].astype(F32) - mean) * inv
            hid_t[p, rows_at(c, CH), :] = (normed * gain_rows(c, CH)).astype(BF16)

        loop(chunks, norm)

        def pack(m):
            part = dot_nn(wqkv_t[rows_at(m, 480), :], hid_t[p])
            pk_t[p, rows_at(m, 480), :] = part.astype(BF16)

        loop(packed // 480, pack)
        keep = lax.broadcasted_iota(jnp.int32, (slots, slots), 0) < count
        for h in range(HEADS):
            q = pk_t[p, rows_at(h, HDIM), :]
            k = pk_t[p, rows_at(h + HEADS, HDIM), :]
            v = pk_t[p, rows_at(h + 2 * HEADS, HDIM), :]
            s = jnp.where(keep, dot_nn(k.T, q), -1e30)
            e = jnp.exp((s - jnp.max(s, axis=0, keepdims=True)) * scale)
            half = (e * (1.0 / jnp.sum(e, axis=0, keepdims=True))).astype(BF16)
            prob_h[p, h] = half
            attn_t[p, rows_at(h, HDIM), :] = dot_nn(v, half).astype(BF16)

    def take_cotangent(p, c):
        count = counts_ref[arrival_ref[p]]
        keep = (lax.broadcasted_iota(jnp.int32, (1, slots), 1) < count).astype(F32)
        piece = cot_ref[:, rows_at(c, PIECE)].T.astype(F32) * keep
        g_recv[p, rows_at(c, PIECE), :] = piece.astype(BF16)

    def hop(p, c):
        return pltpu.make_async_remote_copy(
            src_ref=g_send.at[lax.rem(p, 2), rows_at(c, PIECE)],
            dst_ref=g_recv.at[p, rows_at(c, PIECE)],
            send_sem=send_sem.at[p, c],
            recv_sem=recv_sem.at[p, c],
            device_id={"section": below},
            device_id_type=MESH,
        )

    def backward(p):
        @pl.when(top)
        def _():
            load_cot(p).wait()

        for c in range(pieces):

            @pl.when(top)
            def _():
                take_cotangent(p, c)

            @pl.when(jnp.logical_not(top))
            def _():
                hop(p, c).wait_recv()

            part = dot_nn(wo_t[:, rows_at(c, PIECE)], g_recv[p, rows_at(c, PIECE), :])
            if c == 0:
                ga_acc[...] = part
            elif c < pieces - 1:
                ga_acc[...] += part
            else:
                ga_t[...] = (ga_acc[...] + part).astype(BF16)

        @pl.when(top & (p < micro - 1))
        def _():
            load_cot(p + 1).start()

        first = jnp.zeros((8, slots), F32)
        second = jnp.zeros((8, slots), F32)
        for h in range(HEADS):
            q = pk_t[p, rows_at(h, HDIM), :]
            k = pk_t[p, rows_at(h + HEADS, HDIM), :]
            v = pk_t[p, rows_at(h + 2 * HEADS, HDIM), :]
            ga = ga_t[rows_at(h, HDIM), :]
            half = prob_h[p, h]
            prob = half.astype(F32)
            grad_prob = dot_nn(v.T, ga)
            inner = jnp.sum(prob * grad_prob, axis=0, keepdims=True)
            gs = (prob * (grad_prob - inner)).astype(BF16)
            grads = (dot_nn(k, gs) * scale, dot_nt(q, gs) * scale, dot_nt(ga, half))
            for i, (grad, own) in enumerate(zip(grads, (q, k, v))):
                at = rows_at(h + i * HEADS, HDIM)
                rounded = grad.astype(BF16)
                gpk_t[at, :] = rounded
                full = rounded.astype(F32)
                w = gain_w[at, :]
                first += fold(full * jnp.concatenate([w] * (slots // 128), axis=1))
                second += fold(full * own.astype(F32))
        return (
            jnp.sum(first, axis=0, keepdims=True),
            jnp.sum(second, axis=0, keepdims=True) * (1.0 / width),
        )

    def pass_down(p, first, second):
        inv = stats[p, 0:1, :]
        mean = stats[p, 1:2, :]

        @pl.when(p >= 2)
        def _():
            for c in range(pieces):
                if c != TURN:
                    hop(p - 2, c).wait_send()

        def grad_hidden(c):
            at = rows_at(c, PIECE)
            gn = dot_nn(wqkv_ref[at, :], gpk_t[...]) * gain_rows(c, PIECE)
            normed = (x_t[p, at, :].astype(F32) - mean) * inv
            grad_ln = inv * (gn - first - normed * second)
            g_send[lax.rem(p, 2), at, :] = (g_recv[p, at, :].astype(F32) + grad_ln).astype(BF16)
            hop(p, c).start()

        loop(pieces, grad_hidden)

    def tile(p, n):
        if isinstance(n, int) and n == whole:
            half = dot_nt(hid_t[p], gpk_t[n * TILE : packed, :])
            return jnp.concatenate([half, dot_nt(g_recv[p], attn_t[p, 0:edge, :])], axis=1)
        if isinstance(n, int) and n > whole:
            start = edge + (n - whole - 1) * TILE
            return dot_nt(g_recv[p], attn_t[p, start : start + TILE, :])
        return dot_nt(hid_t[p], gpk_t[rows_at(n, TILE), :])

    def weights(p):
        def qkv(n):
            acc[n] += tile(p, n)

        loop(whole, qkv)
        for n in range(whole, tiles):
            acc[n] += tile(p, n)

    def send(src, dst, i, lane_to):
        return pltpu.make_async_remote_copy(
            src_ref=src,
            dst_ref=dst,
            send_sem=rs_send.at[i],
            recv_sem=rs_recv.at[i],
            device_id={"dp": lane_to},
            device_id_type=MESH,
        )

    nx, ny = TX, tiles - TX
    hx, hy = nx // 2, ny // 2
    at_y1 = tiles
    at_x1 = at_y1 + ny
    at_x2 = at_x1 + nx
    at_x3 = at_x2 + 2 * nx
    at_y2 = at_x3 + nx
    at_y3 = at_y2 + ny
    ways = ((to_right, right), (to_left, left))

    def give_twin(n):
        return send(stage.at[n, :, :, 1 - core], got_a.at[n], n, twin)

    def copy_x1(n):
        way = n // hx
        return send(
            stage.at[n, far, :, core], got_x1.at[way, n % hx], at_x1 + n, ways[way][0]
        )

    def copy_x2(way, n):
        to, block = ways[way]
        return send(stage.at[n, block, :, core], got_x2.at[way, n], at_x2 + way * nx + n, to)

    def copy_x3(n):
        return send(send_x3.at[n], got_x3.at[n], at_x3 + n, to_row)

    def copy_y1(i):
        return send(stage.at[nx + i, :, 1 - row, core], got_y1.at[i], at_y1 + i, to_row)

    def copy_y2(i):
        way = i // hy
        return send(
            stage.at[nx + i, far, row, core], got_y2.at[way, i % hy], at_y2 + i, ways[way][0]
        )

    def copy_y3(way, i):
        to, block = ways[way]
        return send(
            stage.at[nx + i, block, row, core], got_y3.at[way, i], at_y3 + way * ny + i, to
        )

    def join(at, other):
        stage[at] = (stage[at].astype(F32) + other.astype(F32)).astype(BF16)

    def arrive(n):
        give_twin(n).wait_recv()
        for c in range(cols):
            join((n, c, slice(None), core), got_a[n, c])
        if n < nx:
            copy_x1(n).start()
        else:
            copy_y1(n - nx).start()

    def x_second(n):
        way = n // hx
        copy_x1(n).wait_recv()
        copy_x2(1 - way, n).start()
        join((n, ways[way][1], slice(None), core), got_x1[way, n % hx])
        copy_x2(way, n).start()

    def across(n, r):
        total = stage[n, col, r, core].astype(F32) + got_x2[0, n, r].astype(F32)
        return total + got_x2[1, n, r].astype(F32)

    def x_third(n):
        copy_x2(0, n).wait_recv()
        copy_x2(1, n).wait_recv()
        send_x3[n] = across(n, 1 - row).astype(BF16)
        copy_x3(n).start()

    def x_last(n):
        copy_x3(n).wait_recv()
        out_ref[:, n * TILE : (n + 1) * TILE] = across(n, row) + got_x3[n].astype(F32)

    def y_first(i):
        copy_y1(i).wait_recv()
        for c in range(cols):
            join((nx + i, c, row, core), got_y1[i, c])
        copy_y2(i).start()
        copy_y3(1 - i // hy, i).start()

    def y_second(i):
        way = i // hy
        copy_y2(i).wait_recv()
        join((nx + i, ways[way][1], row, core), got_y2[way, i % hy])
        copy_y3(way, i).start()

    def y_last(i):
        copy_y3(0, i).wait_recv()
        copy_y3(1, i).wait_recv()
        n = nx + i
        total = stage[n, col, row, core].astype(F32) + got_y3[0, i].astype(F32)
        out_ref[:, n * TILE : (n + 1) * TILE] = total + got_y3[1, i].astype(F32)

    y_order = [n - nx for n in range(whole, tiles)] + list(range(whole - nx))
    x_order = [h * hx + j for j in range(hx) for h in range(2)]
    order = [nx + i for i in y_order] + x_order

    def last_weights(p):
        for n in order:
            total = (acc[n] + tile(p, n)).astype(BF16)
            stage[n] = total.reshape(stage.shape[1:])
            give_twin(n).start()

            @pl.when(core == 0)
            def _():
                arrive(n)

    def reduce_out():
        @pl.when(core == 1)
        def _():
            for n in order:
                arrive(n)

        pairs = [x_order[2 * j : 2 * j + 2] for j in range(hx)]
        for n in pairs[0]:
            x_second(n)
        y_first(y_order[0])
        for n in pairs[1]:
            x_second(n)
        y_first(y_order[1])
        for n in pairs[2]:
            x_second(n)
        y_second(y_order[0])
        y_first(y_order[2])
        y_second(y_order[1])
        for n in pairs[0]:
            x_third(n)
        y_first(y_order[3])
        y_second(y_order[2])
        for n in pairs[1]:
            x_third(n)
        y_second(y_order[3])
        for n in pairs[2]:
            x_third(n)
        for i in y_order:
            y_last(i)
        for n in x_order:
            x_last(n)
        for n in range(tiles):
            give_twin(n).wait_send()
        for n in range(nx):
            for copy in (copy_x1(n), copy_x2(0, n), copy_x2(1, n), copy_x3(n)):
                copy.wait_send()
        for i in range(ny):
            for copy in (copy_y1(i), copy_y2(i), copy_y3(0, i), copy_y3(1, i)):
                copy.wait_send()

    def clear(c):
        acc[:, rows_at(c, 32), :] = jnp.zeros((tiles, 32, TILE), F32)

    ahead = jnp.minimum(micro, 1 + 2 * (sections - 1 - sec))

    def early(p, carry):
        normalize(p)

        @pl.when(p == 0)
        def _():
            turn_weights()

        attend(p)
        return carry

    lax.fori_loop(0, ahead, early, 0)
    pl.semaphore_wait(barrier, 6)

    def moment(p):
        sums = backward(p)

        @pl.when((sec > 0) & ((core == 0) | (p > 0)))
        def _():
            pl.semaphore_wait(go_sem, 1)

        @pl.when(sec > 0)
        def _():
            pass_down(p, *sums)

        @pl.when(p == 0)
        def _():
            loop(width // 32, clear)

        @pl.when(p < micro - 1)
        def _():
            weights(p)

        @pl.when(p == micro - 1)
        def _():
            last_weights(p)

        @pl.when((sec > 0) & ((core == 1) | (p < micro - 1)))
        def _():
            hop(p, TURN).wait_send()
            pl.semaphore_signal(go_sem, inc=1, device_id={"dp": twin}, device_id_type=MESH)

        @pl.when(p + ahead < micro)
        def _():
            normalize(p + ahead)
            attend(p + ahead)

    loop(micro, moment)
    reduce_out()

    @pl.when(sec > 0)
    def _():
        for p in range(micro - 2, micro):
            for c in range(pieces):
                if c != TURN:
                    hop(p, c).wait_send()

    @pl.when((sec > 0) & (core == 0))
    def _():
        hop(micro - 1, TURN).wait_send()


def run_pipeline(sections, lanes, counts, arrival, x, cotangent, gain, wqkv, wo):
    micro, slots, width = x.shape
    packed, head_span = wqkv.shape[1], wo.shape[1]
    tiles, cols, share = (packed + head_span) // TILE, lanes // 4, width // lanes
    vmem = pl.BlockSpec(memory_space=pltpu.VMEM)
    smem = pl.BlockSpec(memory_space=pltpu.SMEM)
    hbm = pl.BlockSpec(memory_space=pl.ANY)
    pieces = width // PIECE
    scratch = [
        pltpu.VMEM((micro, slots, width), BF16),
        pltpu.VMEM((slots, width), BF16),
        pltpu.VMEM((width, packed), BF16),
        pltpu.VMEM((packed, width), BF16),
        pltpu.VMEM((head_span, width), BF16),
        pltpu.VMEM((width, 128), F32),
        pltpu.VMEM((packed, 128), F32),
        pltpu.VMEM((micro, width, slots), BF16),
        pltpu.VMEM((micro, width, slots), BF16),
        pltpu.VMEM((micro, 8, slots), F32),
        pltpu.VMEM((micro, packed, slots), BF16),
        pltpu.VMEM((micro, HEADS, slots, slots), BF16),
        pltpu.VMEM((micro, head_span, slots), BF16),
        pltpu.VMEM((head_span, slots), BF16),
        pltpu.VMEM((head_span, slots), F32),
        pltpu.VMEM((packed, slots), BF16),
        pltpu.VMEM((tiles, width, TILE), F32),
        pltpu.VMEM((micro, width, slots), BF16),
        pltpu.VMEM((2, width, slots), BF16),
        pltpu.SemaphoreType.DMA((micro, pieces)),
        pltpu.SemaphoreType.DMA((micro, pieces)),
        pltpu.SemaphoreType.REGULAR,
        pltpu.SemaphoreType.DMA((2 + pieces + -(-head_span // PIECE),)),
        pltpu.VMEM((tiles, cols, 2, 2, share, TILE), BF16),
        pltpu.VMEM((tiles, cols, 2, share, TILE), BF16),
        pltpu.VMEM((tiles - TX, cols, share, TILE), BF16),
        pltpu.VMEM((2, TX - TX // 2, 2, share, TILE), BF16),
        pltpu.VMEM((2, TX, 2, share, TILE), BF16),
        pltpu.VMEM((2, tiles - TX - (tiles - TX) // 2, share, TILE), BF16),
        pltpu.VMEM((2, tiles - TX, share, TILE), BF16),
        pltpu.VMEM((TX, share, TILE), BF16),
        pltpu.VMEM((TX, share, TILE), BF16),
        pltpu.SemaphoreType.DMA((tiles + 4 * TX + 4 * (tiles - TX),)),
        pltpu.SemaphoreType.DMA((tiles + 4 * TX + 4 * (tiles - TX),)),
    ]
    return pl.pallas_call(
        functools.partial(pipeline_kernel, sections),
        out_shape=jax.ShapeDtypeStruct((share, packed + head_span), F32),
        in_specs=[smem, smem, hbm, hbm, vmem, hbm, hbm],
        out_specs=vmem,
        scratch_shapes=scratch,
        compiler_params=pltpu.CompilerParams(
            collective_id=0, has_side_effects=True, vmem_limit_bytes=64 * 1024 * 1024 - 65536
        ),
        name="pipeline",
    )(counts, arrival, x, cotangent, gain, wqkv, wo)


def split_kernel(both_ref, qkv_ref, out_ref):
    packed = qkv_ref.shape[1]
    qkv_ref[...] = both_ref[:, :packed]
    out_ref[...] = both_ref[:, packed:]


def per_device(activations, cotangent, counts, arrival, norm_gain, qkv_weight, out_weight):
    sections = lax.axis_size("section")
    packed = qkv_weight.shape[2]
    both = run_pipeline(
        sections,
        lax.axis_size("dp"),
        counts[:, 0],
        arrival,
        activations[0],
        cotangent,
        norm_gain,
        qkv_weight[0],
        out_weight[0],
    )
    share, width = both.shape
    vmem = pl.BlockSpec(memory_space=pltpu.VMEM)
    qkv_share, out_share = pl.pallas_call(
        split_kernel,
        out_shape=(
            jax.ShapeDtypeStruct((share, packed), F32),
            jax.ShapeDtypeStruct((share, width - packed), F32),
        ),
        in_specs=[vmem],
        out_specs=(vmem, vmem),
        name="split",
    )(both)
    return (qkv_share[None], out_share[None])


def solution(mesh):
    placed = (
        P("section", None, "dp", None),
        P(None, "dp", None),
        P(None, "dp"),
        P(),
        P("section", None),
        P("section", None, None),
        P("section", None, None),
    )
    return jax.shard_map(
        per_device,
        mesh=mesh,
        in_specs=placed,
        out_specs=(P("section", "dp", None), P("section", "dp", None)),
        check_vma=False,
    )
```
